16 devices in a mesh: mol: 2 (over y, z), occ: 8 (over x, core).
Axes of the slice: x: 4, y: 2, z: 1, core: 2. Of those that a mesh axis runs over, the one named last changes fastest.
The devices are a block of a 4x4x8 slice.
Arguments:
- b_ints: bfloat16 [672, 80, 152], P(None, ('mol', 'occ')), parts along dimension 1
- eps_occ: float32 [80], P('mol'), parts along dimension 0
- eps_vir: float32 [304], P('mol'), parts along dimension 0
Outputs:
- output 1: float32 [80], P(('mol', 'occ')), parts along dimension 0
- output 2: float32 [2], P('mol'), parts along dimension 0
- output 3: float32 [304, 152], P('mol'), parts along dimension 0
There are 2 independent parts. The reference program is written for one: setup_inputs(seed, part) draws one part's arguments, and reference() takes and returns one part's arrays. A program takes and returns all parts, laid end to end along the dimension named above; each array names one.
All inputs are finite; a program needn't handle non-finite values.
Results may differ from the reference program's by a relative error of at most 0.001.
Values are sent between devices in bfloat16 or wider.
A program may use at most 768 MiB of HBM per device.

```python
import jax
import jax.numpy as jnp
from jax import lax

AUX_DIM = 672
OCC_DIM = 40
VIR_DIM = 152


def setup_inputs(seed: int = 0, part: int = 0) -> dict:
    base_key = jax.random.fold_in(jax.random.key(seed), part)
    key_b, key_gain, key_occ, key_vir = jax.random.split(base_key, 4)
    b_scale = (3.0 / (2.0 * OCC_DIM * VIR_DIM * VIR_DIM * AUX_DIM)) ** 0.25
    orb_gain = jax.random.uniform(key_gain, (OCC_DIM,), jnp.float32, minval=0.6, maxval=1.4)
    b_raw = jax.random.normal(key_b, (AUX_DIM, OCC_DIM, VIR_DIM), jnp.float32)
    b_ints = (b_raw * (orb_gain[None, :, None] * b_scale)).astype(jnp.bfloat16)
    eps_occ = jax.random.uniform(key_occ, (OCC_DIM,), jnp.float32, minval=-1.5, maxval=-0.4)
    eps_vir = jax.random.uniform(key_vir, (VIR_DIM,), jnp.float32, minval=0.2, maxval=2.5)
    return {'b_ints': b_ints, 'eps_occ': eps_occ, 'eps_vir': eps_vir}


def reference(b_ints, eps_occ, eps_vir):
    b_full = b_ints.astype(jnp.float32)
    occ_dim = b_full.shape[1]
    vir_dim = b_full.shape[2]
    vir_sum = eps_vir[:, None] + eps_vir[None, :]

    def one_row(dens_acc, row_idx):
        b_row = lax.dynamic_index_in_dim(b_full, row_idx, axis=1, keepdims=False)
        k_pair = jnp.einsum('qa,qjb->jab', b_row, b_full)
        pair_den = eps_occ[row_idx] + eps_occ[:, None, None] - vir_sum[None]
        t_amp = k_pair / pair_den
        pair_e = jnp.sum(t_amp * (2.0 * k_pair - jnp.swapaxes(k_pair, 1, 2)), axis=(1, 2))
        amp_b = t_amp.astype(jnp.bfloat16).astype(jnp.float32)
        mix_b = (2.0 * t_amp - jnp.swapaxes(t_amp, 1, 2)).astype(jnp.bfloat16).astype(jnp.float32)
        dens_acc = dens_acc + jnp.einsum('jac,jbc->ab', amp_b, mix_b)
        return dens_acc, jnp.sum(pair_e)

    vir_dens, e_pair = lax.scan(one_row, jnp.zeros((vir_dim, vir_dim), jnp.float32), jnp.arange(occ_dim))
    energy = jnp.sum(e_pair).reshape((1,))
    return e_pair, energy, vir_dens
```

```python
import functools

import jax
import jax.numpy as jnp
from jax import lax
from jax.experimental import pallas as pl
from jax.experimental.pallas import tpu as pltpu
from jax.sharding import PartitionSpec as P

MESH_ID = pl.DeviceIdType.MESH
GROUP = 5
CORES = 2
LANES = 256


def flip(bit, by):
    return lax.rem(bit + by, CORES)


def kernel(n_dev, nb, nv, b_ref, eo_ref, ev_ref, dens_ref, epair_ref, energy_ref,
           blk, kbuf, ktbuf, ucat, wcat, vmat, eacc, dacc, rbuf, gbuf,
           load_sem, sib_sem, nbr_send, n_sem, p_sem, red_send, red_recv, gat_send, gat_recv):
    rows = vmat.shape[0]
    n_chip = n_dev // CORES
    me = lax.axis_index('occ')
    chip, core = me // CORES, lax.rem(me, CORES)
    nxt, prv = lax.rem(chip + 1, n_chip), lax.rem(chip + n_chip - 1, n_chip)
    first = lambda c: jnp.where(c == 0, 1, 0)
    n_src = nxt * CORES + flip(core, first(chip))
    p_src = prv * CORES + flip(core, 1 + first(prv))
    n_dst = prv * CORES + flip(core, first(prv))
    p_dst = nxt * CORES + flip(core, 1 + first(chip))
    sib = chip * CORES + flip(core, 1)
    own0, sib0, n0, p0 = 0, nb, 2 * nb, 3 * nb

    load = pltpu.make_async_copy(b_ref, blk.at[pl.ds(own0, nb)], load_sem)
    load.start()
    barrier = pltpu.get_barrier_semaphore()
    for r in range(1, n_dev):
        pl.semaphore_signal(barrier, inc=1, device_id={'occ': lax.rem(me + r, n_dev)}, device_id_type=MESH_ID)

    kbuf[...] = jnp.zeros_like(kbuf)
    ktbuf[...] = jnp.zeros_like(ktbuf)
    wcat[...] = jnp.zeros_like(wcat)
    eacc[...] = jnp.zeros_like(eacc)
    dacc[...] = jnp.zeros_like(dacc)
    vrow = jnp.broadcast_to(ev_ref[...], (nv, nv))
    vmat[...] = jnp.ones_like(vmat)
    vmat[0:nv, 0:nv] = vrow + vrow.T

    load.wait()
    pl.semaphore_wait(barrier, n_dev - 1)

    def remote(src, dst, send, recv, dev):
        return pltpu.make_async_remote_copy(src_ref=src, dst_ref=dst, send_sem=send, recv_sem=recv,
                                            device_id={'occ': dev}, device_id_type=MESH_ID)

    to_n = [remote(blk.at[own0 + s], blk.at[n0 + s], nbr_send.at[0, s], n_sem.at[s], n_dst) for s in range(nb)]
    to_p = [remote(blk.at[own0 + s], blk.at[p0 + s], nbr_send.at[1, s], p_sem.at[s], p_dst) for s in range(nb)]
    to_s = remote(blk.at[pl.ds(own0, nb)], blk.at[pl.ds(sib0, nb)], sib_sem.at[0], sib_sem.at[1], sib)
    for s in range(nb):
        to_n[s].start()
        to_p[s].start()
        if s == 0:
            to_s.start()

    def orb_energy(slot):
        part, off = slot // nb, lax.rem(slot, nb)
        dev = jnp.where(part == 0, me, jnp.where(part == 1, sib, jnp.where(part == 2, n_src, p_src)))
        return eo_ref[dev * nb + off]

    def work(pairs, diag=False):
        for g, (x, y) in enumerate(pairs):
            k_pair = lax.dot_general(blk[x], blk[y], (((1,), (1,)), ((), ())), preferred_element_type=jnp.float32)
            kbuf[g, 0:nv, 0:nv] = k_pair
            ktbuf[g, 0:nv, 0:nv] = k_pair.T
        for g, (x, y) in enumerate(pairs):
            e_sum = orb_energy(x) + orb_energy(y)
            tot = jnp.zeros((16, LANES), jnp.float32)
            for r0 in range(0, rows, 16):
                rs = pl.ds(r0, 16)
                k, kt = kbuf[g, rs, :], ktbuf[g, rs, :]
                rec = 1.0 / (e_sum - vmat[rs, :])
                t, tt = k * rec, kt * rec
                w, wt = (t + t) - tt, (tt + tt) - t
                tot = tot + k * w
                c0 = 2 * g * LANES
                ucat[rs, c0:c0 + LANES] = t.astype(jnp.bfloat16)
                wcat[pl.ds(c0 + r0, 16), :] = wt.astype(jnp.bfloat16)
                if not diag:
                    c1 = c0 + LANES
                    ucat[rs, c1:c1 + LANES] = tt.astype(jnp.bfloat16)
                    wcat[pl.ds(c1 + r0, 16), :] = w.astype(jnp.bfloat16)
            part = tot[0:8, 0:128] + tot[8:16, 0:128] + tot[0:8, 128:256] + tot[8:16, 128:256]
            eacc[x] = eacc[x] + part
            if not diag:
                eacc[y] = eacc[y] + part
        if diag:
            term = sum(jnp.dot(ucat[:, 2 * g * LANES:(2 * g + 1) * LANES], wcat[2 * g * LANES:(2 * g + 1) * LANES, :],
                               preferred_element_type=jnp.float32) for g in range(len(pairs)))
        else:
            depth = 2 * LANES * len(pairs)
            term = jnp.dot(ucat[:, 0:depth], wcat[0:depth, :], preferred_element_type=jnp.float32)
        dacc[0:rows, :] = dacc[0:rows, :] + term

    work([(own0 + i, own0 + i) for i in range(nb)], diag=True)

    def own_step(i, _):
        work([(own0 + i, own0 + lax.rem(i + d, nb)) for d in range(1, nb // 2 + 1)])
        return 0

    lax.fori_loop(0, nb, own_step, 0)

    to_s.wait_recv()

    def sib_pair(i, d):
        j = lax.rem(i + d, nb)
        return own0 + jnp.where(core == 0, i, j), sib0 + jnp.where(core == 0, j, i)

    half = nb // 2

    def sib_step(i, _):
        work([sib_pair(i, d + jnp.where(core == 0, 0, half + 1)) for d in range(half)])
        return 0

    lax.fori_loop(0, nb, sib_step, 0)

    def sib_rest(i, _):
        work([sib_pair(i, half)])
        return 0

    cut = (nb + 1) // 2
    lax.fori_loop(jnp.where(core == 0, 0, cut), jnp.where(core == 0, cut, nb), sib_rest, 0)

    def step(s, _):
        remote(blk.at[own0], blk.at[n0 + s], nbr_send.at[0, s], n_sem.at[s], n_dst).wait_recv()
        remote(blk.at[own0], blk.at[p0 + s], nbr_send.at[1, s], p_sem.at[s], p_dst).wait_recv()
        work([(own0 + i, n0 + s) for i in range(nb)])
        work([(own0 + i, p0 + s) for i in range(nb)])
        work([(n0 + s, p0 + s)])

        def cross(t, _):
            work([(n0 + s, p0 + t), (n0 + t, p0 + s)])
            return 0

        lax.fori_loop(0, s, cross, 0)
        return 0

    lax.fori_loop(0, nb, step, 0)

    lane = lax.broadcasted_iota(jnp.int32, (8, LANES), 1)
    sub = lax.broadcasted_iota(jnp.int32, (8, LANES), 0)
    erow = jnp.zeros((8, LANES), jnp.float32)
    for part, dev in enumerate((me, sib, n_src, p_src)):
        for s in range(nb):
            e_val = jnp.sum(jnp.sum(eacc[part * nb + s], axis=0, keepdims=True), axis=1, keepdims=True)
            erow = erow + jnp.where((lane == dev * nb + s) & (sub == 0), e_val, 0.0)
    dacc[nv:nv + 8, :] = erow

    cut_rows = gbuf.shape[0] // n_dev
    reds, gats = [], []
    for r in range(1, n_dev):
        dst = lax.rem(me + r, n_dev)
        reds.append(remote(dacc.at[pl.ds(dst * cut_rows, cut_rows)], rbuf.at[r - 1], red_send.at[r - 1], red_recv.at[r - 1], dst))
        reds[-1].start()
    mine = pl.ds(me * cut_rows, cut_rows)
    for c in reds:
        c.wait_recv()
    total = dacc[mine, :]
    for r in range(1, n_dev):
        total = total + rbuf[r - 1]
    gbuf[mine, :] = total
    for r in range(1, n_dev):
        dst = lax.rem(me + r, n_dev)
        gats.append(remote(gbuf.at[mine], gbuf.at[mine], gat_send.at[r - 1], gat_recv.at[r - 1], dst))
        gats[-1].start()
    for r in range(1, n_dev):
        src = lax.rem(me + n_dev - r, n_dev)
        remote(gbuf.at[mine], gbuf.at[pl.ds(src * cut_rows, cut_rows)], gat_send.at[r - 1], gat_recv.at[r - 1], src).wait_recv()
    dens_ref[...] = gbuf[0:nv, 0:nv]
    e_all = gbuf[nv:nv + 8, :]
    energy_ref[...] = jnp.sum(jnp.sum(e_all, axis=0, keepdims=True), axis=1, keepdims=True)
    e_mine = pltpu.roll(e_all, lax.rem(LANES - me * nb, LANES), 1)
    epair_ref[...] = e_mine[0:1, 0:nb]
    for c in to_n + to_p + [to_s] + reds + gats:
        c.wait_send()


def solution(mesh):
    n_dev = mesh.shape['occ']

    def per_device(b_blk, eps_occ, eps_vir):
        nq, nb, nv = b_blk.shape
        rows = (nv + 15) // 16 * 16
        cut_rows = (-(-(nv + 8) // n_dev) + 7) // 8 * 8
        by_orb = jnp.transpose(b_blk, (1, 2, 0))
        vmem = pltpu.VMEM
        dma = pltpu.SemaphoreType.DMA
        dens, e_pair, energy = pl.pallas_call(
            functools.partial(kernel, n_dev, nb, nv),
            out_shape=(jax.ShapeDtypeStruct((nv, nv), jnp.float32), jax.ShapeDtypeStruct((1, nb), jnp.float32),
                       jax.ShapeDtypeStruct((1, 1), jnp.float32)),
            in_specs=[pl.BlockSpec(memory_space=pl.ANY), pl.BlockSpec(memory_space=pltpu.SMEM),
                      pl.BlockSpec(memory_space=vmem)],
            out_specs=(pl.BlockSpec(memory_space=vmem),) * 3,
            scratch_shapes=[
                vmem((4 * nb, nv, nq), jnp.bfloat16),
                vmem((GROUP, rows, LANES), jnp.float32),
                vmem((GROUP, rows, LANES), jnp.float32),
                vmem((rows, 2 * GROUP * LANES), jnp.bfloat16),
                vmem((2 * GROUP * LANES, LANES), jnp.bfloat16),
                vmem((rows, LANES), jnp.float32),
                vmem((4 * nb, 8, 128), jnp.float32),
                vmem((n_dev * cut_rows, LANES), jnp.float32),
                vmem((n_dev - 1, cut_rows, LANES), jnp.float32),
                vmem((n_dev * cut_rows, LANES), jnp.float32),
                dma, dma((2,)), dma((2, nb)), dma((nb,)), dma((nb,)),
                dma((n_dev - 1,)), dma((n_dev - 1,)), dma((n_dev - 1,)), dma((n_dev - 1,)),
            ],
            compiler_params=pltpu.CompilerParams(collective_id=0, has_side_effects=True),
        )(by_orb, eps_occ, eps_vir.reshape(1, nv))
        return e_pair.reshape(nb), energy.reshape(1), dens

    return jax.shard_map(per_device, mesh=mesh, in_specs=(P(None, ('mol', 'occ'), None), P('mol'), P('mol')),
                         out_specs=(P(('mol', 'occ')), P('mol'), P('mol', None)), check_vma=False)
```

```python
import functools

import jax
import jax.numpy as jnp
from jax import lax
from jax.experimental import pallas as pl
from jax.experimental.pallas import tpu as pltpu
from jax.sharding import PartitionSpec as P

MESH_ID = pl.DeviceIdType.MESH
CORES = 2
LANES = 128
WIDE = 2 * LANES


def flip(bit, by):
    return lax.rem(bit + by, CORES)


def remote(src, dst, send, recv, dev):
    return pltpu.make_async_remote_copy(src_ref=src, dst_ref=dst, send_sem=send, recv_sem=recv,
                                        device_id={'occ': dev}, device_id_type=MESH_ID)


def kernel(n_dev, nb, nv, nq, b_ref, eo_ref, ev_ref, red_ref, e_ref,
           blk, rem, pack, eo, ev, kbuf, ktbuf, ucat, wcat, vmat, eacc, dacc, part, rbuf, ebuf, elocal,
           load_sem, sib_sem, nbr_send, n_sem, p_sem, red_send, red_recv, gat_send, gat_recv, e_send, e_recv):
    rows = vmat.shape[0]
    main = nq // LANES * LANES
    tail = nq - main
    packed = pack.shape[2]
    n_chip = n_dev // CORES
    me = lax.axis_index('occ')
    chip, core = me // CORES, lax.rem(me, CORES)
    nxt, prv = lax.rem(chip + 1, n_chip), lax.rem(chip + n_chip - 1, n_chip)
    first = lambda c: jnp.where(c == 0, 1, 0)
    n_src = nxt * CORES + flip(core, first(chip))
    p_src = prv * CORES + flip(core, 1 + first(prv))
    n_dst = prv * CORES + flip(core, first(prv))
    p_dst = nxt * CORES + flip(core, 1 + first(chip))
    sib = chip * CORES + flip(core, 1)
    own0, sib0, n0, p0 = 0, nb, 2 * nb, 3 * nb

    barrier = pltpu.get_barrier_semaphore()
    for r in range(1, n_dev):
        pl.semaphore_signal(barrier, inc=1, device_id={'occ': lax.rem(me + r, n_dev)}, device_id_type=MESH_ID)
    loads = [pltpu.make_async_copy(b_ref.at[:, :, main:nq], rem, load_sem.at[0]),
             pltpu.make_async_copy(b_ref.at[:, :, 0:main], blk.at[pl.ds(own0, nb), 0:nv, 0:main], load_sem.at[1]),
             pltpu.make_async_copy(eo_ref, eo, load_sem.at[2]),
             pltpu.make_async_copy(ev_ref, ev, load_sem.at[3])]
    for c in loads:
        c.start()

    for s in range(4 * nb):
        blk[s, nv:rows, :] = jnp.zeros((rows - nv, blk.shape[2]), jnp.bfloat16)
    kbuf[...] = jnp.zeros_like(kbuf)
    ktbuf[...] = jnp.zeros_like(ktbuf)
    wcat[...] = jnp.zeros_like(wcat)
    eacc[...] = jnp.zeros_like(eacc)
    dacc[...] = jnp.zeros_like(dacc)
    part[...] = jnp.zeros_like(part)

    lane = lax.broadcasted_iota(jnp.int32, (packed, LANES), 1)
    groups = LANES // tail
    loads[0].wait()
    for s in range(nb):
        own_tail = jnp.concatenate([rem[s].astype(jnp.float32), jnp.zeros((nv, LANES - tail), jnp.float32)], axis=1)
        blk[own0 + s, 0:nv, main:main + LANES] = own_tail.astype(jnp.bfloat16)
        filled = jnp.concatenate([own_tail, jnp.zeros((groups * packed - nv, LANES), jnp.float32)], axis=0)
        mix = filled[0:packed]
        for g in range(1, groups):
            mix = mix + pltpu.roll(filled[g * packed:(g + 1) * packed], g * tail, 1)
        pack[0, s] = mix.astype(jnp.bfloat16)
    loads[2].wait()
    loads[3].wait()
    vrow = jnp.broadcast_to(ev[...], (nv, nv))
    vmat[...] = jnp.ones_like(vmat)
    vmat[0:nv, 0:nv] = vrow + vrow.T
    loads[1].wait()
    pl.semaphore_wait(barrier, n_dev - 1)

    def cols(slot):
        return blk.at[slot, 0:nv, 0:main]

    to_n = [remote(pack.at[0], pack.at[1], nbr_send.at[0, nb], n_sem.at[nb], n_dst)]
    to_p = [remote(pack.at[0], pack.at[2], nbr_send.at[1, nb], p_sem.at[nb], p_dst)]
    to_s = [remote(pack.at[0], pack.at[3], sib_sem.at[0, 0], sib_sem.at[1, 0], sib),
            remote(blk.at[pl.ds(own0, nb), 0:nv, 0:main], blk.at[pl.ds(sib0, nb), 0:nv, 0:main],
                   sib_sem.at[0, 1], sib_sem.at[1, 1], sib)]
    to_n += [remote(cols(own0 + s), cols(n0 + s), nbr_send.at[0, s], n_sem.at[s], n_dst) for s in range(nb)]
    to_p += [remote(cols(own0 + s), cols(p0 + s), nbr_send.at[1, s], p_sem.at[s], p_dst) for s in range(nb)]
    for s in range(nb + 1):
        to_n[s].start()
        to_p[s].start()
        if s == 1:
            to_s[0].start()
            to_s[1].start()

    def unpack(which, slot0):
        for s in range(nb):
            mix = pack[which, s].astype(jnp.float32)
            parts = [mix] + [pltpu.roll(mix, LANES - g * tail, 1) for g in range(1, groups)]
            full = jnp.concatenate([jnp.where(lane < tail, q, 0.0) for q in parts], axis=0)
            blk[slot0 + s, :, main:main + LANES] = full.astype(jnp.bfloat16)

    def orb_energy(slot):
        if isinstance(slot, int):
            dev = (me, sib, n_src, p_src)[slot // nb]
            return eo[dev * nb + slot % nb]
        kind, off = slot // nb, lax.rem(slot, nb)
        dev = jnp.where(kind == 0, me, jnp.where(kind == 1, sib, jnp.where(kind == 2, n_src, p_src)))
        return eo[dev * nb + off]

    def work(pairs, diag=(), weight=None):
        c0 = 0
        for g, (x, y) in enumerate(pairs):
            k_pair = lax.dot_general(blk[x], blk[y], (((1,), (1,)), ((), ())), preferred_element_type=jnp.float32)
            kbuf[g, :, 0:rows] = k_pair
            ktbuf[g, :, 0:rows] = k_pair.T
            e_sum = orb_energy(x) + orb_energy(y)
            tot = jnp.zeros((16, WIDE), jnp.float32)
            for r0 in range(0, rows, 16):
                rs = pl.ds(r0, 16)
                k, kt = kbuf[g, rs, :], ktbuf[g, rs, :]
                rec = 1.0 / (e_sum - vmat[rs, :])
                if weight is not None and g in weight:
                    rec = rec * weight[g]
                t, tt = k * rec, kt * rec
                w, wt = (t + t) - tt, (tt + tt) - t
                tot = tot + k * w
                ucat[rs, c0:c0 + WIDE] = t.astype(jnp.bfloat16)
                wcat[pl.ds(c0 + r0, 16), :] = wt.astype(jnp.bfloat16)
                if g not in diag:
                    c1 = c0 + WIDE
                    ucat[rs, c1:c1 + WIDE] = tt.astype(jnp.bfloat16)
                    wcat[pl.ds(c1 + r0, 16), :] = w.astype(jnp.bfloat16)
            c0 += WIDE if g in diag else 2 * WIDE
            fold = tot[0:8, 0:LANES] + tot[8:16, 0:LANES] + tot[0:8, LANES:WIDE] + tot[8:16, LANES:WIDE]
            eacc[x] = eacc[x] + fold
            if g not in diag:
                eacc[y] = eacc[y] + fold
        dacc[...] = dacc[...] + jnp.dot(ucat[:, 0:c0], wcat[0:c0, :], preferred_element_type=jnp.float32)

    ring = nb // 2
    work([(own0 + i, own0 + i) for i in range(nb)]
         + [(own0 + i, own0 + (i + d) % nb) for d in range(1, ring + 1) for i in range(nb)], diag=range(nb))

    to_s[0].wait_recv()
    unpack(3, sib0)
    to_s[1].wait_recv()

    def sib_pair(i, d):
        j = lax.rem(i + d, nb)
        return own0 + jnp.where(core == 0, i, j), sib0 + jnp.where(core == 0, j, i)

    shift = jnp.where(core == 0, 0, ring + 1)
    cut = (nb + 1) // 2
    rest = [(jnp.where(core == 0, i, jnp.minimum(cut + i, nb - 1)), ring) for i in range(cut)]
    work([sib_pair(i, d + shift) for d in range(ring) for i in range(nb)] + [sib_pair(i, d) for i, d in rest],
         weight={ring * nb + cut - 1: jnp.where(core == 0, 1.0, 0.0)})

    def arrive(s):
        remote(cols(own0), cols(n0 + s), nbr_send.at[0, s], n_sem.at[s], n_dst).wait_recv()
        remote(cols(own0), cols(p0 + s), nbr_send.at[1, s], p_sem.at[s], p_dst).wait_recv()

    def fresh(s):
        return ([(own0 + i, n0 + s) for i in range(nb)] + [(own0 + i, p0 + s) for i in range(nb)] + [(n0 + s, p0 + s)])

    to_n[0].wait_recv()
    unpack(1, n0)
    to_p[0].wait_recv()
    unpack(2, p0)

    def step(s, _):
        arrive(s)
        work(fresh(s))

        def cross(t, _):
            work([(n0 + s, p0 + t), (n0 + t, p0 + s)])
            return 0

        lax.fori_loop(0, s, cross, 0)
        return 0

    lax.fori_loop(0, nb - 1, step, 0)
    last = nb - 1
    arrive(last)
    work(fresh(last) + [q for t in range(last) for q in ((n0 + last, p0 + t), (n0 + t, p0 + last))])

    extra = nv - LANES
    stack = 32
    part[0:nv, :] = dacc[0:nv, 0:LANES]
    lane32 = lax.broadcasted_iota(jnp.int32, (stack, LANES), 1)
    side = dacc[:, LANES:WIDE]
    mix = side[0:stack]
    for g in range(1, rows // stack):
        mix = mix + pltpu.roll(side[g * stack:(g + 1) * stack], g * extra, 1)
    part[nv:nv + stack, :] = mix

    cut_rows = red_ref.shape[0] // n_dev
    reds, gats, es = [], [], []
    for r in range(1, n_dev):
        dst = lax.rem(me + r, n_dev)
        reds.append(remote(part.at[pl.ds(dst * cut_rows, cut_rows)], rbuf.at[r - 1], red_send.at[r - 1], red_recv.at[r - 1], dst))
        reds[-1].start()

    lane1 = lax.broadcasted_iota(jnp.int32, (1, LANES), 1)
    erow = jnp.zeros((1, LANES), jnp.float32)
    for kind, dev in enumerate((me, sib, n_src, p_src)):
        for s in range(nb):
            e_val = jnp.sum(jnp.sum(eacc[kind * nb + s], axis=0, keepdims=True), axis=1, keepdims=True)
            erow = erow + jnp.where(lane1 == dev * nb + s, e_val, 0.0)
    elocal[...] = erow
    for r in range(1, n_dev):
        es.append(remote(elocal, ebuf.at[r - 1], e_send.at[r - 1], e_recv.at[r - 1], lax.rem(me + r, n_dev)))
        es[-1].start()

    mine = pl.ds(me * cut_rows, cut_rows)
    for c in reds:
        c.wait_recv()
    total = part[mine, :]
    for r in range(1, n_dev):
        total = total + rbuf[r - 1]
    red_ref[mine, :] = total
    for r in range(1, n_dev):
        dst = lax.rem(me + r, n_dev)
        gats.append(remote(red_ref.at[mine], red_ref.at[mine], gat_send.at[r - 1], gat_recv.at[r - 1], dst))
        gats[-1].start()
    for c in es:
        c.wait_recv()
    place = lax.rem(me, n_dev)
    e_all = jnp.zeros((1, LANES), jnp.float32)
    for d in range(n_dev):
        took = elocal[...]
        for r in range(1, n_dev):
            took = jnp.where(lax.rem(place + n_dev - r, n_dev) == d, ebuf[r - 1], took)
        e_all = e_all + took
    e_ref[0:1, :] = pltpu.roll(jnp.broadcast_to(e_all, (8, LANES)), lax.rem(LANES - me * nb, LANES), 1)[0:1]
    e_ref[1:2, :] = jnp.broadcast_to(jnp.sum(e_all, axis=1, keepdims=True), (1, LANES))
    for r in range(1, n_dev):
        src = lax.rem(me + n_dev - r, n_dev)
        remote(red_ref.at[mine], red_ref.at[pl.ds(src * cut_rows, cut_rows)], gat_send.at[r - 1], gat_recv.at[r - 1], src).wait_recv()
    for c in to_n + to_p + to_s + reds + gats + es:
        c.wait_send()


def finish(nb, nv, red_ref, e_ref, dens_ref, epair_ref, energy_ref):
    extra, stack = nv - LANES, 32
    dens_ref[:, 0:LANES] = red_ref[0:nv, :]
    mix = red_ref[nv:nv + stack, :]
    for g in range(-(-nv // stack)):
        n = min(stack, nv - g * stack)
        side = mix if g == 0 else pltpu.roll(mix, LANES - g * extra, 1)
        dens_ref[g * stack:g * stack + n, LANES:nv] = side[0:n, 0:extra]
    epair_ref[...] = e_ref[0:1, 0:nb]
    energy_ref[...] = e_ref[1:2, 0:1]


def solution(mesh):
    n_dev = mesh.shape['occ']

    def per_device(b_blk, eps_occ, eps_vir):
        nq, nb, nv = b_blk.shape
        rows = (nv + 15) // 16 * 16
        n_cut = -(-(nv + 32) // n_dev)
        cut_rows = (n_cut + 7) // 8 * 8
        deep = (nq + LANES - 1) // LANES * LANES
        most = max(3 * nb, 4 * nb - 1)
        by_orb = jnp.transpose(b_blk, (1, 2, 0))
        vmem = pltpu.VMEM
        dma = pltpu.SemaphoreType.DMA
        f32, bf16 = jnp.float32, jnp.bfloat16
        anyspace = pl.BlockSpec(memory_space=pl.ANY)
        in_vmem = pl.BlockSpec(memory_space=vmem)
        red, e_rows = pl.pallas_call(
            functools.partial(kernel, n_dev, nb, nv, nq),
            out_shape=(jax.ShapeDtypeStruct((n_dev * cut_rows, LANES), f32), jax.ShapeDtypeStruct((8, LANES), f32)),
            in_specs=[anyspace] * 3,
            out_specs=(in_vmem,) * 2,
            scratch_shapes=[
                vmem((4 * nb, rows, deep), bf16),
                vmem((nb, nv, nq % LANES), bf16),
                vmem((4, nb, rows // (LANES // (nq % LANES)), LANES), bf16),
                pltpu.SMEM((nb * n_dev,), f32),
                vmem((1, nv), f32),
                vmem((most, rows, WIDE), f32),
                vmem((most, rows, WIDE), f32),
                vmem((rows, 2 * most * WIDE), bf16),
                vmem((2 * most * WIDE, WIDE), bf16),
                vmem((rows, WIDE), f32),
                vmem((4 * nb, 8, LANES), f32),
                vmem((rows, WIDE), f32),
                vmem((n_dev * cut_rows, LANES), f32),
                vmem((n_dev - 1, cut_rows, LANES), f32),
                vmem((n_dev - 1, 1, LANES), f32),
                vmem((1, LANES), f32),
                dma((4,)), dma((2, 2)), dma((2, nb + 1)), dma((nb + 1,)), dma((nb + 1,)),
                dma((n_dev - 1,)), dma((n_dev - 1,)), dma((n_dev - 1,)), dma((n_dev - 1,)),
                dma((n_dev - 1,)), dma((n_dev - 1,)),
            ],
            compiler_params=pltpu.CompilerParams(collective_id=0, has_side_effects=True),
        )(by_orb, eps_occ, eps_vir.reshape(1, nv))
        dens, e_pair, energy = pl.pallas_call(
            functools.partial(finish, nb, nv),
            out_shape=(jax.ShapeDtypeStruct((nv, nv), f32), jax.ShapeDtypeStruct((1, nb), f32), jax.ShapeDtypeStruct((1, 1), f32)),
            in_specs=[in_vmem] * 2,
            out_specs=(in_vmem,) * 3,
        )(red, e_rows)
        return e_pair.reshape(nb), energy.reshape(1), dens

    return jax.shard_map(per_device, mesh=mesh, in_specs=(P(None, ('mol', 'occ'), None), P('mol'), P('mol')),
                         out_specs=(P(('mol', 'occ')), P('mol'), P('mol', None)), check_vma=False)
```

```python
import functools

import jax
import jax.numpy as jnp
from jax import lax
from jax.experimental import pallas as pl
from jax.experimental.pallas import tpu as pltpu
from jax.sharding import PartitionSpec as P

MESH_ID = pl.DeviceIdType.MESH
CORES = 2
LANES = 128
WIDE = 2 * LANES


def flip(bit, by):
    return lax.rem(bit + by, CORES)


def remote(src, dst, send, recv, dev):
    return pltpu.make_async_remote_copy(src_ref=src, dst_ref=dst, send_sem=send, recv_sem=recv,
                                        device_id={'occ': dev}, device_id_type=MESH_ID)


def kernel(n_dev, nb, nv, nq, b_ref, eo_ref, ev_ref, red_ref, e_ref,
           blk, rem, pack, eo, ev, kbuf, ktbuf, ucat, wcat, vmat, eacc, dacc, part, rbuf, ebuf, elocal,
           load_sem, sib_sem, nbr_send, nbr_sem, red_send, red_recv, gat_send, gat_recv, e_send, e_recv):
    rows = vmat.shape[0]
    main = nq // LANES * LANES
    tail = nq - main
    packed = pack.shape[2]
    n_chip = n_dev // CORES
    me = lax.axis_index('occ')
    chip, core = me // CORES, lax.rem(me, CORES)
    nxt, prv = lax.rem(chip + 1, n_chip), lax.rem(chip + n_chip - 1, n_chip)
    first = lambda c: jnp.where(c == 0, 1, 0)
    n_src = nxt * CORES + flip(core, first(chip))
    p_src = prv * CORES + flip(core, 1 + first(prv))
    n_dst = prv * CORES + flip(core, first(prv))
    p_dst = nxt * CORES + flip(core, 1 + first(chip))
    sib = chip * CORES + flip(core, 1)
    own0, sib0, e0, l0 = 0, nb, 2 * nb, 3 * nb
    n_early = core == 0
    p_early = core == flip(first(chip), first(nxt))
    got_n_early = flip(core, first(chip)) == 0
    e_src = jnp.where(got_n_early, n_src, p_src)
    l_src = jnp.where(got_n_early, p_src, n_src)

    barrier = pltpu.get_barrier_semaphore()
    for r in range(1, n_dev):
        pl.semaphore_signal(barrier, inc=1, device_id={'occ': lax.rem(me + r, n_dev)}, device_id_type=MESH_ID)
    loads = [pltpu.make_async_copy(b_ref.at[:, :, main:nq], rem, load_sem.at[0]),
             pltpu.make_async_copy(b_ref.at[:, :, 0:main], blk.at[pl.ds(own0, nb), 0:nv, 0:main], load_sem.at[1]),
             pltpu.make_async_copy(eo_ref, eo, load_sem.at[2]),
             pltpu.make_async_copy(ev_ref, ev, load_sem.at[3])]
    for c in loads:
        c.start()

    for s in range(4 * nb):
        blk[s, nv:rows, :] = jnp.zeros((rows - nv, blk.shape[2]), jnp.bfloat16)
    for g in range(kbuf.shape[0]):
        kbuf[g, :, LANES:WIDE] = jnp.zeros((rows, LANES), jnp.float32)
        ktbuf[g, :, LANES:WIDE] = jnp.zeros((rows, LANES), jnp.float32)
    for g in range(wcat.shape[0] // WIDE):
        wcat[g * WIDE + rows:(g + 1) * WIDE, :] = jnp.zeros((WIDE - rows, WIDE), jnp.bfloat16)
    eacc[...] = jnp.zeros_like(eacc)
    dacc[...] = jnp.zeros_like(dacc)
    part[...] = jnp.zeros_like(part)

    lane = lax.broadcasted_iota(jnp.int32, (packed, LANES), 1)
    groups = LANES // tail
    loads[0].wait()
    for s in range(nb):
        own_tail = jnp.concatenate([rem[s].astype(jnp.float32), jnp.zeros((nv, LANES - tail), jnp.float32)], axis=1)
        blk[own0 + s, 0:nv, main:main + LANES] = own_tail.astype(jnp.bfloat16)
        filled = jnp.concatenate([own_tail, jnp.zeros((groups * packed - nv, LANES), jnp.float32)], axis=0)
        mix = filled[0:packed]
        for g in range(1, groups):
            mix = mix + pltpu.roll(filled[g * packed:(g + 1) * packed], g * tail, 1)
        pack[0, s] = mix.astype(jnp.bfloat16)
    loads[2].wait()
    loads[3].wait()
    vrow = jnp.broadcast_to(ev[...], (nv, nv))
    vmat[...] = jnp.ones_like(vmat)
    vmat[0:nv, 0:nv] = vrow + vrow.T
    loads[1].wait()
    pl.semaphore_wait(barrier, n_dev - 1)

    def cols(slot):
        return blk.at[slot, 0:nv, 0:main]

    def flow(which, early, dst):
        late = jnp.where(early, 0, 1)
        return ([remote(cols(own0 + s), cols(e0 + late * nb + s), nbr_send.at[which, s], nbr_sem.at[late, s], dst)
                 for s in range(nb)]
                + [remote(pack.at[0], pack.at[1 + late], nbr_send.at[which, nb], nbr_sem.at[late, nb], dst)])

    to_n, to_p = flow(0, n_early, n_dst), flow(1, p_early, p_dst)
    to_s = [remote(pack.at[0], pack.at[3], sib_sem.at[0, 0], sib_sem.at[1, 0], sib),
            remote(blk.at[pl.ds(own0, nb), 0:nv, 0:main], blk.at[pl.ds(sib0, nb), 0:nv, 0:main],
                   sib_sem.at[0, 1], sib_sem.at[1, 1], sib)]

    def launch(copies, when):
        @pl.when(when)
        def _():
            for c in copies:
                c.start()

    to_n[nb].start()
    to_p[nb].start()
    launch(to_n[0:nb], n_early)
    launch(to_p[0:nb], p_early)
    for c in to_s:
        c.start()

    def unpack(which, slot0):
        for s in range(nb):
            mix = pack[which, s].astype(jnp.float32)
            parts = [mix] + [pltpu.roll(mix, LANES - g * tail, 1) for g in range(1, groups)]
            full = jnp.concatenate([jnp.where(lane < tail, q, 0.0) for q in parts], axis=0)
            blk[slot0 + s, :, main:main + LANES] = full.astype(jnp.bfloat16)

    def orb_energy(slot):
        if isinstance(slot, int):
            dev = (me, sib, e_src, l_src)[slot // nb]
            return eo[dev * nb + slot % nb]
        kind, off = slot // nb, lax.rem(slot, nb)
        dev = jnp.where(kind == 0, me, jnp.where(kind == 1, sib, jnp.where(kind == 2, e_src, l_src)))
        return eo[dev * nb + off]

    def work(pairs, diag=(), weight=None):
        c0 = 0
        for g, (x, y) in enumerate(pairs):
            k_pair = lax.dot_general(blk[x], blk[y], (((1,), (1,)), ((), ())), preferred_element_type=jnp.float32)
            kbuf[g, :, 0:rows] = k_pair
            ktbuf[g, :, 0:rows] = k_pair.T
            e_sum = orb_energy(x) + orb_energy(y)
            tot = jnp.zeros((16, WIDE), jnp.float32)
            for r0 in range(0, rows, 16):
                rs = pl.ds(r0, 16)
                k, kt = kbuf[g, rs, :], ktbuf[g, rs, :]
                rec = 1.0 / (e_sum - vmat[rs, :])
                if weight is not None and g in weight:
                    rec = rec * weight[g]
                t, tt = k * rec, kt * rec
                w, wt = (t + t) - tt, (tt + tt) - t
                tot = tot + k * w
                ucat[rs, c0:c0 + WIDE] = t.astype(jnp.bfloat16)
                wcat[pl.ds(c0 + r0, 16), :] = wt.astype(jnp.bfloat16)
                if g not in diag:
                    c1 = c0 + WIDE
                    ucat[rs, c1:c1 + WIDE] = tt.astype(jnp.bfloat16)
                    wcat[pl.ds(c1 + r0, 16), :] = w.astype(jnp.bfloat16)
            c0 += WIDE if g in diag else 2 * WIDE
            fold = tot[0:8, 0:LANES] + tot[8:16, 0:LANES] + tot[0:8, LANES:WIDE] + tot[8:16, LANES:WIDE]
            eacc[x] = eacc[x] + fold
            if g not in diag:
                eacc[y] = eacc[y] + fold
        dacc[...] = dacc[...] + jnp.dot(ucat[:, 0:c0], wcat[0:c0, :], preferred_element_type=jnp.float32)

    ring = nb // 2
    work([(own0 + i, own0 + i) for i in range(nb)]
         + [(own0 + i, own0 + (i + d) % nb) for d in range(1, ring + 1) for i in range(nb)], diag=range(nb))

    to_s[0].wait_recv()
    unpack(3, sib0)
    to_s[1].wait_recv()

    def sib_pair(i, d):
        j = lax.rem(i + d, nb)
        return own0 + jnp.where(core == 0, i, j), sib0 + jnp.where(core == 0, j, i)

    shift = jnp.where(core == 0, 0, ring + 1)
    cut = (nb + 1) // 2
    rest = [(jnp.where(core == 0, i, jnp.minimum(cut + i, nb - 1)), ring) for i in range(cut)]
    work([sib_pair(i, d + shift) for d in range(ring) for i in range(nb)] + [sib_pair(i, d) for i, d in rest],
         weight={ring * nb + cut - 1: jnp.where(core == 0, 1.0, 0.0)})

    launch(to_n[0:nb], jnp.logical_not(n_early))
    launch(to_p[0:nb], jnp.logical_not(p_early))

    def arrive(late, s):
        remote(cols(own0), cols(e0 + late * nb + s), nbr_send.at[0, s], nbr_sem.at[late, s], n_dst).wait_recv()

    def arrive_rest(late):
        remote(pack.at[0], pack.at[1 + late], nbr_send.at[0, nb], nbr_sem.at[late, nb], n_dst).wait_recv()
        unpack(1 + late, e0 + late * nb)

    def with_own(slot):
        return [(own0 + i, slot) for i in range(nb)]

    head = nb // 2
    arrive_rest(0)
    for s in range(head):
        arrive(0, s)
    work([q for s in range(head) for q in with_own(e0 + s)])
    arrive_rest(1)
    for j in range(nb - head):
        arrive(0, head + j)
        arrive(1, j)
        work(with_own(e0 + head + j) + with_own(l0 + j) + [(e0 + s, l0 + j) for s in range(head + j + 1)]
             + [(e0 + head + j, l0 + s) for s in range(j)])

    def late_step(j, _):
        arrive(1, j)
        work(with_own(l0 + j) + [(e0 + s, l0 + j) for s in range(nb)])
        return 0

    lax.fori_loop(nb - head, nb, late_step, 0)

    extra = nv - LANES
    stack = 32
    part[0:nv, :] = dacc[0:nv, 0:LANES]
    lane32 = lax.broadcasted_iota(jnp.int32, (stack, LANES), 1)
    side = dacc[:, LANES:WIDE]
    mix = side[0:stack]
    for g in range(1, rows // stack):
        mix = mix + pltpu.roll(side[g * stack:(g + 1) * stack], g * extra, 1)
    part[nv:nv + stack, :] = mix

    cut_rows = red_ref.shape[0] // n_dev
    reds, gats, es = [], [], []
    for r in range(1, n_dev):
        dst = lax.rem(me + r, n_dev)
        reds.append(remote(part.at[pl.ds(dst * cut_rows, cut_rows)], rbuf.at[r - 1], red_send.at[r - 1], red_recv.at[r - 1], dst))
        reds[-1].start()

    lane1 = lax.broadcasted_iota(jnp.int32, (1, LANES), 1)
    erow = jnp.zeros((1, LANES), jnp.float32)
    for kind, dev in enumerate((me, sib, e_src, l_src)):
        for s in range(nb):
            e_val = jnp.sum(jnp.sum(eacc[kind * nb + s], axis=0, keepdims=True), axis=1, keepdims=True)
            erow = erow + jnp.where(lane1 == dev * nb + s, e_val, 0.0)
    elocal[...] = erow
    for r in range(1, n_dev):
        es.append(remote(elocal, ebuf.at[r - 1], e_send.at[r - 1], e_recv.at[r - 1], lax.rem(me + r, n_dev)))
        es[-1].start()

    mine = pl.ds(me * cut_rows, cut_rows)
    for c in reds:
        c.wait_recv()
    total = part[mine, :]
    for r in range(1, n_dev):
        total = total + rbuf[r - 1]
    red_ref[mine, :] = total
    for r in range(1, n_dev):
        dst = lax.rem(me + r, n_dev)
        gats.append(remote(red_ref.at[mine], red_ref.at[mine], gat_send.at[r - 1], gat_recv.at[r - 1], dst))
        gats[-1].start()
    for c in es:
        c.wait_recv()
    place = lax.rem(me, n_dev)
    e_all = jnp.zeros((1, LANES), jnp.float32)
    for d in range(n_dev):
        took = elocal[...]
        for r in range(1, n_dev):
            took = jnp.where(lax.rem(place + n_dev - r, n_dev) == d, ebuf[r - 1], took)
        e_all = e_all + took
    e_ref[0:1, :] = pltpu.roll(jnp.broadcast_to(e_all, (8, LANES)), lax.rem(LANES - me * nb, LANES), 1)[0:1]
    e_ref[1:2, :] = jnp.broadcast_to(jnp.sum(e_all, axis=1, keepdims=True), (1, LANES))
    for r in range(1, n_dev):
        src = lax.rem(me + n_dev - r, n_dev)
        remote(red_ref.at[mine], red_ref.at[pl.ds(src * cut_rows, cut_rows)], gat_send.at[r - 1], gat_recv.at[r - 1], src).wait_recv()
    for c in to_n + to_p + to_s + reds + gats + es:
        c.wait_send()


def finish(nb, nv, red_ref, e_ref, dens_ref, epair_ref, energy_ref):
    extra, stack = nv - LANES, 32
    dens_ref[:, 0:LANES] = red_ref[0:nv, :]
    mix = red_ref[nv:nv + stack, :]
    for g in range(-(-nv // stack)):
        n = min(stack, nv - g * stack)
        side = mix if g == 0 else pltpu.roll(mix, LANES - g * extra, 1)
        dens_ref[g * stack:g * stack + n, LANES:nv] = side[0:n, 0:extra]
    epair_ref[...] = e_ref[0:1, 0:nb]
    energy_ref[...] = e_ref[1:2, 0:1]


def solution(mesh):
    n_dev = mesh.shape['occ']

    def per_device(b_blk, eps_occ, eps_vir):
        nq, nb, nv = b_blk.shape
        rows = (nv + 15) // 16 * 16
        n_cut = -(-(nv + 32) // n_dev)
        cut_rows = (n_cut + 7) // 8 * 8
        deep = (nq + LANES - 1) // LANES * LANES
        most = 3 * nb + nb // 2
        by_orb = jnp.transpose(b_blk, (1, 2, 0))
        vmem = pltpu.VMEM
        dma = pltpu.SemaphoreType.DMA
        f32, bf16 = jnp.float32, jnp.bfloat16
        anyspace = pl.BlockSpec(memory_space=pl.ANY)
        in_vmem = pl.BlockSpec(memory_space=vmem)
        red, e_rows = pl.pallas_call(
            functools.partial(kernel, n_dev, nb, nv, nq),
            out_shape=(jax.ShapeDtypeStruct((n_dev * cut_rows, LANES), f32), jax.ShapeDtypeStruct((8, LANES), f32)),
            in_specs=[anyspace] * 3,
            out_specs=(in_vmem,) * 2,
            scratch_shapes=[
                vmem((4 * nb, rows, deep), bf16),
                vmem((nb, nv, nq % LANES), bf16),
                vmem((4, nb, rows // (LANES // (nq % LANES)), LANES), bf16),
                pltpu.SMEM((nb * n_dev,), f32),
                vmem((1, nv), f32),
                vmem((most, rows, WIDE), f32),
                vmem((most, rows, WIDE), f32),
                vmem((rows, 2 * most * WIDE), bf16),
                vmem((2 * most * WIDE, WIDE), bf16),
                vmem((rows, WIDE), f32),
                vmem((4 * nb, 8, LANES), f32),
                vmem((rows, WIDE), f32),
                vmem((n_dev * cut_rows, LANES), f32),
                vmem((n_dev - 1, cut_rows, LANES), f32),
                vmem((n_dev - 1, 1, LANES), f32),
                vmem((1, LANES), f32),
                dma((4,)), dma((2, 2)), dma((2, nb + 1)), dma((2, nb + 1)),
                dma((n_dev - 1,)), dma((n_dev - 1,)), dma((n_dev - 1,)), dma((n_dev - 1,)),
                dma((n_dev - 1,)), dma((n_dev - 1,)),
            ],
            compiler_params=pltpu.CompilerParams(collective_id=0, has_side_effects=True),
        )(by_orb, eps_occ, eps_vir.reshape(1, nv))
        dens, e_pair, energy = pl.pallas_call(
            functools.partial(finish, nb, nv),
            out_shape=(jax.ShapeDtypeStruct((nv, nv), f32), jax.ShapeDtypeStruct((1, nb), f32), jax.ShapeDtypeStruct((1, 1), f32)),
            in_specs=[in_vmem] * 2,
            out_specs=(in_vmem,) * 3,
        )(red, e_rows)
        return e_pair.reshape(nb), energy.reshape(1), dens

    return jax.shard_map(per_device, mesh=mesh, in_specs=(P(None, ('mol', 'occ'), None), P('mol'), P('mol')),
                         out_specs=(P(('mol', 'occ')), P('mol'), P('mol', None)), check_vma=False)
```

```python
import functools

import jax
import jax.numpy as jnp
from jax import lax
from jax.experimental import pallas as pl
from jax.experimental.pallas import tpu as pltpu
from jax.sharding import PartitionSpec as P

MESH_ID = pl.DeviceIdType.MESH
CORES = 2
LANES = 128
WIDE = 2 * LANES


def flip(bit, by):
    return lax.rem(bit + by, CORES)


def remote(src, dst, send, recv, dev):
    return pltpu.make_async_remote_copy(src_ref=src, dst_ref=dst, send_sem=send, recv_sem=recv,
                                        device_id={'occ': dev}, device_id_type=MESH_ID)


def kernel(n_dev, nb, nv, nq, b_ref, eo_ref, ev_ref, red_ref, e_ref,
           blk, rem, pack, eo, ev, kbuf, ktbuf, ucat, wcat, vmat, eacc, dacc, part, rbuf, ebuf, elocal,
           load_sem, sib_sem, nbr_send, nbr_sem, red_send, red_recv, gat_send, gat_recv, e_send, e_recv):
    rows = vmat.shape[0]
    main = nq // LANES * LANES
    tail = nq - main
    packed = pack.shape[2]
    n_chip = n_dev // CORES
    me = lax.axis_index('occ')
    chip, core = me // CORES, lax.rem(me, CORES)
    nxt, prv = lax.rem(chip + 1, n_chip), lax.rem(chip + n_chip - 1, n_chip)
    first = lambda c: jnp.where(c == 0, 1, 0)
    n_src = nxt * CORES + flip(core, first(chip))
    p_src = prv * CORES + flip(core, 1 + first(prv))
    n_dst = prv * CORES + flip(core, first(prv))
    p_dst = nxt * CORES + flip(core, 1 + first(chip))
    sib = chip * CORES + flip(core, 1)
    own0, sib0, e0, l0 = 0, nb, 2 * nb, 3 * nb
    n_early = core == 0
    p_early = core == flip(first(chip), first(nxt))
    got_n_early = flip(core, first(chip)) == 0
    e_src = jnp.where(got_n_early, n_src, p_src)
    l_src = jnp.where(got_n_early, p_src, n_src)

    barrier = pltpu.get_barrier_semaphore()
    for r in range(1, n_dev):
        pl.semaphore_signal(barrier, inc=1, device_id={'occ': lax.rem(me + r, n_dev)}, device_id_type=MESH_ID)
    loads = [pltpu.make_async_copy(b_ref.at[:, :, main:nq], rem, load_sem.at[0]),
             pltpu.make_async_copy(b_ref.at[:, :, 0:main], blk.at[pl.ds(own0, nb), 0:nv, 0:main], load_sem.at[1]),
             pltpu.make_async_copy(eo_ref, eo, load_sem.at[2]),
             pltpu.make_async_copy(ev_ref, ev, load_sem.at[3])]
    for c in loads:
        c.start()

    for s in range(4 * nb):
        blk[s, nv:rows, :] = jnp.zeros((rows - nv, blk.shape[2]), jnp.bfloat16)
    for g in range(kbuf.shape[0]):
        kbuf[g, :, LANES:WIDE] = jnp.zeros((rows, LANES), jnp.float32)
        ktbuf[g, :, LANES:WIDE] = jnp.zeros((rows, LANES), jnp.float32)
    for g in range(wcat.shape[0] // WIDE):
        wcat[g * WIDE + rows:(g + 1) * WIDE, :] = jnp.zeros((WIDE - rows, WIDE), jnp.bfloat16)
    eacc[...] = jnp.zeros_like(eacc)
    dacc[...] = jnp.zeros_like(dacc)
    part[...] = jnp.zeros_like(part)

    lane = lax.broadcasted_iota(jnp.int32, (packed, LANES), 1)
    groups = LANES // tail
    loads[0].wait()
    for s in range(nb):
        own_tail = jnp.concatenate([rem[s].astype(jnp.float32), jnp.zeros((nv, LANES - tail), jnp.float32)], axis=1)
        blk[own0 + s, 0:nv, main:main + LANES] = own_tail.astype(jnp.bfloat16)
        filled = jnp.concatenate([own_tail, jnp.zeros((groups * packed - nv, LANES), jnp.float32)], axis=0)
        mix = filled[0:packed]
        for g in range(1, groups):
            mix = mix + pltpu.roll(filled[g * packed:(g + 1) * packed], g * tail, 1)
        pack[0, s] = mix.astype(jnp.bfloat16)
    loads[2].wait()
    loads[3].wait()
    vrow = jnp.broadcast_to(ev[...], (nv, nv))
    vmat[...] = jnp.ones_like(vmat)
    vmat[0:nv, 0:nv] = vrow + vrow.T
    loads[1].wait()
    pl.semaphore_wait(barrier, n_dev - 1)

    def cols(slot):
        return blk.at[slot, 0:nv, 0:main]

    def flow(which, early, dst):
        late = jnp.where(early, 0, 1)
        return ([remote(cols(own0 + s), cols(e0 + late * nb + s), nbr_send.at[which, s], nbr_sem.at[late, s], dst)
                 for s in range(nb)]
                + [remote(pack.at[0], pack.at[1 + late], nbr_send.at[which, nb], nbr_sem.at[late, nb], dst)])

    to_n, to_p = flow(0, n_early, n_dst), flow(1, p_early, p_dst)
    to_s = [remote(pack.at[0], pack.at[3], sib_sem.at[0, 0], sib_sem.at[1, 0], sib),
            remote(blk.at[pl.ds(own0, nb), 0:nv, 0:main], blk.at[pl.ds(sib0, nb), 0:nv, 0:main],
                   sib_sem.at[0, 1], sib_sem.at[1, 1], sib)]

    def launch(copies, when):
        @pl.when(when)
        def _():
            for c in copies:
                c.start()

    to_n[nb].start()
    to_p[nb].start()
    launch(to_n[0:nb], n_early)
    launch(to_p[0:nb], p_early)
    for c in to_s:
        c.start()

    def unpack(which, slot0):
        for s in range(nb):
            mix = pack[which, s].astype(jnp.float32)
            parts = [mix] + [pltpu.roll(mix, LANES - g * tail, 1) for g in range(1, groups)]
            full = jnp.concatenate([jnp.where(lane < tail, q, 0.0) for q in parts], axis=0)
            blk[slot0 + s, :, main:main + LANES] = full.astype(jnp.bfloat16)

    def orb_energy(slot):
        if isinstance(slot, int):
            dev = (me, sib, e_src, l_src)[slot // nb]
            return eo[dev * nb + slot % nb]
        kind, off = slot // nb, lax.rem(slot, nb)
        dev = jnp.where(kind == 0, me, jnp.where(kind == 1, sib, jnp.where(kind == 2, e_src, l_src)))
        return eo[dev * nb + off]

    def work(pairs, diag=(), weight=None):
        c0 = 0
        for g, (x, y) in enumerate(pairs):
            k_pair = lax.dot_general(blk[x], blk[y], (((1,), (1,)), ((), ())), preferred_element_type=jnp.float32)
            kbuf[g, :, 0:rows] = k_pair
            ktbuf[g, :, 0:rows] = k_pair.T
            e_sum = orb_energy(x) + orb_energy(y)
            tot = jnp.zeros((16, WIDE), jnp.float32)
            for r0 in range(0, rows, 16):
                rs = pl.ds(r0, 16)
                k, kt = kbuf[g, rs, :], ktbuf[g, rs, :]
                rec = 1.0 / (e_sum - vmat[rs, :])
                if weight is not None and g in weight:
                    rec = rec * weight[g]
                t, tt = k * rec, kt * rec
                w, wt = (t + t) - tt, (tt + tt) - t
                tot = tot + k * w
                ucat[rs, c0:c0 + WIDE] = t.astype(jnp.bfloat16)
                wcat[pl.ds(c0 + r0, 16), :] = wt.astype(jnp.bfloat16)
                if g not in diag:
                    c1 = c0 + WIDE
                    ucat[rs, c1:c1 + WIDE] = tt.astype(jnp.bfloat16)
                    wcat[pl.ds(c1 + r0, 16), :] = w.astype(jnp.bfloat16)
            c0 += WIDE if g in diag else 2 * WIDE
            fold = tot[0:8, 0:LANES] + tot[8:16, 0:LANES] + tot[0:8, LANES:WIDE] + tot[8:16, LANES:WIDE]
            eacc[x] = eacc[x] + fold
            if g not in diag:
                eacc[y] = eacc[y] + fold
        dacc[...] = dacc[...] + jnp.dot(ucat[:, 0:c0], wcat[0:c0, :], preferred_element_type=jnp.float32)

    ring = nb // 2
    work([(own0 + i, own0 + i) for i in range(nb)]
         + [(own0 + i, own0 + (i + d) % nb) for d in range(1, ring + 1) for i in range(nb)], diag=range(nb))

    to_s[0].wait_recv()
    unpack(3, sib0)
    to_s[1].wait_recv()

    def sib_pair(i, d):
        j = lax.rem(i + d, nb)
        return own0 + jnp.where(core == 0, i, j), sib0 + jnp.where(core == 0, j, i)

    shift = jnp.where(core == 0, 0, ring + 1)
    cut = (nb + 1) // 2
    rest = [(jnp.where(core == 0, i, jnp.minimum(cut + i, nb - 1)), ring) for i in range(cut)]
    work([sib_pair(i, d + shift) for d in range(ring) for i in range(nb)] + [sib_pair(i, d) for i, d in rest],
         weight={ring * nb + cut - 1: jnp.where(core == 0, 1.0, 0.0)})

    def arrive(late, s):
        remote(cols(own0), cols(e0 + late * nb + s), nbr_send.at[0, s], nbr_sem.at[late, s], n_dst).wait_recv()

    def arrive_rest(late):
        remote(pack.at[0], pack.at[1 + late], nbr_send.at[0, nb], nbr_sem.at[late, nb], n_dst).wait_recv()
        unpack(1 + late, e0 + late * nb)

    def with_own(slot):
        return [(own0 + i, slot) for i in range(nb)]

    head = nb // 2
    arrive_rest(0)
    for s in range(head):
        arrive(0, s)
    work([q for s in range(head) for q in with_own(e0 + s)])
    arrive(0, head)
    work(with_own(e0 + head))
    launch(to_n[0:nb], jnp.logical_not(n_early))
    launch(to_p[0:nb], jnp.logical_not(p_early))

    for s in range(head + 1, nb):
        arrive(0, s)
    work([q for s in range(head + 1, nb) for q in with_own(e0 + s)])
    arrive_rest(1)

    def late_step(j, _):
        arrive(1, j)
        work(with_own(l0 + j) + [(e0 + s, l0 + j) for s in range(nb)])
        return 0

    lax.fori_loop(0, nb, late_step, 0)

    extra = nv - LANES
    stack = 32
    part[0:nv, :] = dacc[0:nv, 0:LANES]
    lane32 = lax.broadcasted_iota(jnp.int32, (stack, LANES), 1)
    side = dacc[:, LANES:WIDE]
    mix = side[0:stack]
    for g in range(1, rows // stack):
        mix = mix + pltpu.roll(side[g * stack:(g + 1) * stack], g * extra, 1)
    part[nv:nv + stack, :] = mix

    cut_rows = red_ref.shape[0] // n_dev
    reds, gats, es = [], [], []
    order = sorted(range(1, n_dev), key=lambda r: -min(r, n_dev - r))
    for r in order:
        dst = lax.rem(me + r, n_dev)
        reds.append(remote(part.at[pl.ds(dst * cut_rows, cut_rows)], rbuf.at[r - 1], red_send.at[r - 1], red_recv.at[r - 1], dst))
        reds[-1].start()

    lane1 = lax.broadcasted_iota(jnp.int32, (1, LANES), 1)
    erow = jnp.zeros((1, LANES), jnp.float32)
    for kind, dev in enumerate((me, sib, e_src, l_src)):
        for s in range(nb):
            e_val = jnp.sum(jnp.sum(eacc[kind * nb + s], axis=0, keepdims=True), axis=1, keepdims=True)
            erow = erow + jnp.where(lane1 == dev * nb + s, e_val, 0.0)
    elocal[...] = erow
    for r in range(1, n_dev):
        es.append(remote(elocal, ebuf.at[r - 1], e_send.at[r - 1], e_recv.at[r - 1], lax.rem(me + r, n_dev)))
        es[-1].start()

    mine = pl.ds(me * cut_rows, cut_rows)
    for c in reds:
        c.wait_recv()
    total = part[mine, :]
    for r in range(1, n_dev):
        total = total + rbuf[r - 1]
    red_ref[mine, :] = total
    for r in order:
        dst = lax.rem(me + r, n_dev)
        gats.append(remote(red_ref.at[mine], red_ref.at[mine], gat_send.at[r - 1], gat_recv.at[r - 1], dst))
        gats[-1].start()
    for c in es:
        c.wait_recv()
    place = lax.rem(me, n_dev)
    e_all = jnp.zeros((1, LANES), jnp.float32)
    for d in range(n_dev):
        took = elocal[...]
        for r in range(1, n_dev):
            took = jnp.where(lax.rem(place + n_dev - r, n_dev) == d, ebuf[r - 1], took)
        e_all = e_all + took
    e_ref[0:1, :] = pltpu.roll(jnp.broadcast_to(e_all, (8, LANES)), lax.rem(LANES - me * nb, LANES), 1)[0:1]
    e_ref[1:2, :] = jnp.broadcast_to(jnp.sum(e_all, axis=1, keepdims=True), (1, LANES))
    for r in range(1, n_dev):
        src = lax.rem(me + n_dev - r, n_dev)
        remote(red_ref.at[mine], red_ref.at[pl.ds(src * cut_rows, cut_rows)], gat_send.at[r - 1], gat_recv.at[r - 1], src).wait_recv()
    for c in to_n + to_p + to_s + reds + gats + es:
        c.wait_send()


def finish(nb, nv, red_ref, e_ref, dens_ref, epair_ref, energy_ref):
    extra, stack = nv - LANES, 32
    dens_ref[:, 0:LANES] = red_ref[0:nv, :]
    mix = red_ref[nv:nv + stack, :]
    for g in range(-(-nv // stack)):
        n = min(stack, nv - g * stack)
        side = mix if g == 0 else pltpu.roll(mix, LANES - g * extra, 1)
        dens_ref[g * stack:g * stack + n, LANES:nv] = side[0:n, 0:extra]
    epair_ref[...] = e_ref[0:1, 0:nb]
    energy_ref[...] = e_ref[1:2, 0:1]


def solution(mesh):
    n_dev = mesh.shape['occ']

    def per_device(b_blk, eps_occ, eps_vir):
        nq, nb, nv = b_blk.shape
        rows = (nv + 15) // 16 * 16
        n_cut = -(-(nv + 32) // n_dev)
        cut_rows = (n_cut + 7) // 8 * 8
        deep = (nq + LANES - 1) // LANES * LANES
        most = 3 * nb
        by_orb = jnp.transpose(b_blk, (1, 2, 0))
        vmem = pltpu.VMEM
        dma = pltpu.SemaphoreType.DMA
        f32, bf16 = jnp.float32, jnp.bfloat16
        anyspace = pl.BlockSpec(memory_space=pl.ANY)
        in_vmem = pl.BlockSpec(memory_space=vmem)
        red, e_rows = pl.pallas_call(
            functools.partial(kernel, n_dev, nb, nv, nq),
            out_shape=(jax.ShapeDtypeStruct((n_dev * cut_rows, LANES), f32), jax.ShapeDtypeStruct((8, LANES), f32)),
            in_specs=[anyspace] * 3,
            out_specs=(in_vmem,) * 2,
            scratch_shapes=[
                vmem((4 * nb, rows, deep), bf16),
                vmem((nb, nv, nq % LANES), bf16),
                vmem((4, nb, rows // (LANES // (nq % LANES)), LANES), bf16),
                pltpu.SMEM((nb * n_dev,), f32),
                vmem((1, nv), f32),
                vmem((most, rows, WIDE), f32),
                vmem((most, rows, WIDE), f32),
                vmem((rows, 2 * most * WIDE), bf16),
                vmem((2 * most * WIDE, WIDE), bf16),
                vmem((rows, WIDE), f32),
                vmem((4 * nb, 8, LANES), f32),
                vmem((rows, WIDE), f32),
                vmem((n_dev * cut_rows, LANES), f32),
                vmem((n_dev - 1, cut_rows, LANES), f32),
                vmem((n_dev - 1, 1, LANES), f32),
                vmem((1, LANES), f32),
                dma((4,)), dma((2, 2)), dma((2, nb + 1)), dma((2, nb + 1)),
                dma((n_dev - 1,)), dma((n_dev - 1,)), dma((n_dev - 1,)), dma((n_dev - 1,)),
                dma((n_dev - 1,)), dma((n_dev - 1,)),
            ],
            compiler_params=pltpu.CompilerParams(collective_id=0, has_side_effects=True),
        )(by_orb, eps_occ, eps_vir.reshape(1, nv))
        dens, e_pair, energy = pl.pallas_call(
            functools.partial(finish, nb, nv),
            out_shape=(jax.ShapeDtypeStruct((nv, nv), f32), jax.ShapeDtypeStruct((1, nb), f32), jax.ShapeDtypeStruct((1, 1), f32)),
            in_specs=[in_vmem] * 2,
            out_specs=(in_vmem,) * 3,
        )(red, e_rows)
        return e_pair.reshape(nb), energy.reshape(1), dens

    return jax.shard_map(per_device, mesh=mesh, in_specs=(P(None, ('mol', 'occ'), None), P('mol'), P('mol')),
                         out_specs=(P(('mol', 'occ')), P('mol'), P('mol', None)), check_vma=False)
```

```python
import functools

import jax
import jax.numpy as jnp
from jax import lax
from jax.experimental import pallas as pl
from jax.experimental.pallas import tpu as pltpu
from jax.sharding import PartitionSpec as P

MESH_ID = pl.DeviceIdType.MESH
CORES = 2
LANES = 128
WIDE = 2 * LANES


def flip(bit, by):
    return lax.rem(bit + by, CORES)


def remote(src, dst, send, recv, dev):
    return pltpu.make_async_remote_copy(src_ref=src, dst_ref=dst, send_sem=send, recv_sem=recv,
                                        device_id={'occ': dev}, device_id_type=MESH_ID)


def kernel(n_dev, nb, nv, nq, b_ref, eo_ref, ev_ref, red_ref, e_ref,
           blk, rem, pack, eo, ev, kbuf, ktbuf, ucat, wcat, vmat, eacc, dacc, part, rbuf, ebuf, elocal,
           ypt, kp, ktp, up, wp, vrest,
           load_sem, sib_sem, nbr_send, nbr_sem, red_send, red_recv, gat_send, gat_recv, e_send, e_recv):
    rows = vmat.shape[0]
    main = nq // LANES * LANES
    deep = blk.shape[2]
    tail = nq - main
    packed = pack.shape[2]
    n_chip = n_dev // CORES
    me = lax.axis_index('occ')
    chip, core = me // CORES, lax.rem(me, CORES)
    nxt, prv = lax.rem(chip + 1, n_chip), lax.rem(chip + n_chip - 1, n_chip)
    first = lambda c: jnp.where(c == 0, 1, 0)
    n_src = nxt * CORES + flip(core, first(chip))
    p_src = prv * CORES + flip(core, 1 + first(prv))
    n_dst = prv * CORES + flip(core, first(prv))
    p_dst = nxt * CORES + flip(core, 1 + first(chip))
    sib = chip * CORES + flip(core, 1)
    own0, sib0, e0, l0 = 0, nb, 2 * nb, 3 * nb
    n_early = core == 0
    p_early = core == flip(first(chip), first(nxt))
    got_n_early = flip(core, first(chip)) == 0
    e_src = jnp.where(got_n_early, n_src, p_src)
    l_src = jnp.where(got_n_early, p_src, n_src)

    barrier = pltpu.get_barrier_semaphore()
    for r in range(1, n_dev):
        pl.semaphore_signal(barrier, inc=1, device_id={'occ': lax.rem(me + r, n_dev)}, device_id_type=MESH_ID)
    loads = [pltpu.make_async_copy(b_ref.at[:, :, main:nq], rem, load_sem.at[0]),
             pltpu.make_async_copy(b_ref.at[:, :, 0:main], blk.at[pl.ds(own0, nb), 0:nv, 0:main], load_sem.at[1]),
             pltpu.make_async_copy(eo_ref, eo, load_sem.at[2]),
             pltpu.make_async_copy(ev_ref, ev, load_sem.at[3])]
    for c in loads:
        c.start()

    for s in range(4 * nb):
        blk[s, nv:rows, :] = jnp.zeros((rows - nv, blk.shape[2]), jnp.bfloat16)
    for g in range(kbuf.shape[0]):
        kbuf[g, :, LANES:WIDE] = jnp.zeros((rows, LANES), jnp.float32)
        ktbuf[g, :, LANES:WIDE] = jnp.zeros((rows, LANES), jnp.float32)
    for g in range(wcat.shape[0] // WIDE):
        wcat[g * WIDE + rows:(g + 1) * WIDE, :] = jnp.zeros((WIDE - rows, WIDE), jnp.bfloat16)
    eacc[...] = jnp.zeros_like(eacc)
    dacc[...] = jnp.zeros_like(dacc)
    part[...] = jnp.zeros_like(part)

    lane = lax.broadcasted_iota(jnp.int32, (packed, LANES), 1)
    groups = LANES // tail
    loads[0].wait()
    for s in range(nb):
        own_tail = jnp.concatenate([rem[s].astype(jnp.float32), jnp.zeros((nv, LANES - tail), jnp.float32)], axis=1)
        blk[own0 + s, 0:nv, main:main + LANES] = own_tail.astype(jnp.bfloat16)
        filled = jnp.concatenate([own_tail, jnp.zeros((groups * packed - nv, LANES), jnp.float32)], axis=0)
        mix = filled[0:packed]
        for g in range(1, groups):
            mix = mix + pltpu.roll(filled[g * packed:(g + 1) * packed], g * tail, 1)
        pack[0, s] = mix.astype(jnp.bfloat16)
    loads[2].wait()
    loads[3].wait()
    vrow = jnp.broadcast_to(ev[...], (nv, nv))
    vmat[...] = jnp.ones_like(vmat)
    vmat[0:nv, 0:nv] = vrow + vrow.T
    loads[1].wait()
    pl.semaphore_wait(barrier, n_dev - 1)

    def cols(slot):
        return blk.at[slot, 0:nv, 0:main]

    def flow(which, early, dst):
        late = jnp.where(early, 0, 1)
        return ([remote(cols(own0 + s), cols(e0 + late * nb + s), nbr_send.at[which, s], nbr_sem.at[late, s], dst)
                 for s in range(nb)]
                + [remote(pack.at[0], pack.at[1 + late], nbr_send.at[which, nb], nbr_sem.at[late, nb], dst)])

    to_n, to_p = flow(0, n_early, n_dst), flow(1, p_early, p_dst)
    to_s = [remote(pack.at[0], pack.at[3], sib_sem.at[0, 0], sib_sem.at[1, 0], sib),
            remote(blk.at[pl.ds(own0, nb), 0:nv, 0:main], blk.at[pl.ds(sib0, nb), 0:nv, 0:main],
                   sib_sem.at[0, 1], sib_sem.at[1, 1], sib)]

    def launch(copies, when):
        @pl.when(when)
        def _():
            for c in copies:
                c.start()

    to_n[nb].start()
    to_p[nb].start()
    launch(to_n[0:nb], n_early)
    launch(to_p[0:nb], p_early)
    for c in to_s:
        c.start()

    def unpack(which, slot0):
        for s in range(nb):
            mix = pack[which, s].astype(jnp.float32)
            parts = [mix] + [pltpu.roll(mix, LANES - g * tail, 1) for g in range(1, groups)]
            full = jnp.concatenate([jnp.where(lane < tail, q, 0.0) for q in parts], axis=0)
            blk[slot0 + s, :, main:main + LANES] = full.astype(jnp.bfloat16)

    def orb_energy(slot):
        if isinstance(slot, int):
            dev = (me, sib, e_src, l_src)[slot // nb]
            return eo[dev * nb + slot % nb]
        kind, off = slot // nb, lax.rem(slot, nb)
        dev = jnp.where(kind == 0, me, jnp.where(kind == 1, sib, jnp.where(kind == 2, e_src, l_src)))
        return eo[dev * nb + off]

    def work(pairs, diag=(), weight=None):
        c0 = 0
        for g, (x, y) in enumerate(pairs):
            k_pair = lax.dot_general(blk[x], blk[y], (((1,), (1,)), ((), ())), preferred_element_type=jnp.float32)
            kbuf[g, :, 0:rows] = k_pair
            ktbuf[g, :, 0:rows] = k_pair.T
            e_sum = orb_energy(x) + orb_energy(y)
            tot = jnp.zeros((16, WIDE), jnp.float32)
            for r0 in range(0, rows, 16):
                rs = pl.ds(r0, 16)
                k, kt = kbuf[g, rs, :], ktbuf[g, rs, :]
                rec = 1.0 / (e_sum - vmat[rs, :])
                if weight is not None and g in weight:
                    rec = rec * weight[g]
                t, tt = k * rec, kt * rec
                w, wt = (t + t) - tt, (tt + tt) - t
                tot = tot + k * w
                ucat[rs, c0:c0 + WIDE] = t.astype(jnp.bfloat16)
                wcat[pl.ds(c0 + r0, 16), :] = wt.astype(jnp.bfloat16)
                if g not in diag:
                    c1 = c0 + WIDE
                    ucat[rs, c1:c1 + WIDE] = tt.astype(jnp.bfloat16)
                    wcat[pl.ds(c1 + r0, 16), :] = w.astype(jnp.bfloat16)
            c0 += WIDE if g in diag else 2 * WIDE
            fold = tot[0:8, 0:LANES] + tot[8:16, 0:LANES] + tot[0:8, LANES:WIDE] + tot[8:16, LANES:WIDE]
            eacc[x] = eacc[x] + fold
            if g not in diag:
                eacc[y] = eacc[y] + fold
        dacc[...] = dacc[...] + jnp.dot(ucat[:, 0:c0], wcat[0:c0, :], preferred_element_type=jnp.float32)

    extra = nv - LANES
    tiles = nb + 1
    band = tiles * LANES
    side = nb * LANES
    lane128 = lax.broadcasted_iota(jnp.int32, (1, LANES), 1)

    def in_band(j):
        return (lane128 >= j * extra) & (lane128 < (j + 1) * extra)

    def pack_rows(which, s0):
        for n in range(nb):
            ypt[which, :, n * LANES:(n + 1) * LANES] = blk[s0 + n, 0:LANES, :].astype(jnp.float32).T.astype(jnp.bfloat16)
        rests = [blk[s0 + n, LANES:rows, :].astype(jnp.float32)[0:extra] for n in range(nb)]
        rests.append(jnp.zeros((LANES - nb * extra, deep), jnp.float32))
        ypt[which, :, side:band] = jnp.concatenate(rests, axis=0).T.astype(jnp.bfloat16)

    def late_group(g, x, s0):
        kp[g] = jnp.dot(blk[x], ypt[g], preferred_element_type=jnp.float32)
        side_t = kp[g, 0:LANES, side:band].T
        for n in range(nb):
            at = pl.ds(n * LANES, LANES)
            ktp[g, 0:LANES, at] = kp[g, 0:LANES, at].T
            ktp[g, LANES:nv, at] = side_t[n * extra:(n + 1) * extra]
        low = [kp[g, LANES:nv, n * LANES:(n + 1) * LANES] for n in range(nb)]
        low.append(jnp.zeros((LANES - nb * extra, LANES), jnp.float32))
        ktp[g, 0:LANES, side:band] = jnp.concatenate(low, axis=0).T
        corner = kp[g, LANES:nv, side:band]
        corner_t = jnp.concatenate([corner, jnp.zeros((LANES - extra, LANES), jnp.float32)], axis=0).T
        spread = corner_t[0:extra]
        for n in range(1, nb):
            spread = spread + pltpu.roll(corner_t[n * extra:(n + 1) * extra], n * extra, 1)
        ktp[g, LANES:nv, side:band] = spread
        e_x = orb_energy(x)
        e_sums = [e_x + orb_energy(s0 + n) for n in range(nb)]
        e_rest = jnp.full((1, LANES), e_sums[nb - 1], jnp.float32)
        for n in range(nb - 1):
            e_rest = jnp.where(in_band(n), e_sums[n], e_rest)
        tots = [jnp.zeros((16, LANES), jnp.float32) for _ in range(tiles)]
        c0 = 2 * g * band
        for r0 in range(0, rows, 16):
            rs = pl.ds(r0, 16)
            for n in range(tiles):
                k, kt = kp[g, rs, n * LANES:(n + 1) * LANES], ktp[g, rs, n * LANES:(n + 1) * LANES]
                den = e_rest - vrest[rs, :] if n == nb else e_sums[n] - vmat[rs, 0:LANES]
                rec = 1.0 / den
                t, tt = k * rec, kt * rec
                w, wt = (t + t) - tt, (tt + tt) - t
                tots[n] = tots[n] + k * w
                c = c0 + n * LANES
                up[rs, c:c + LANES] = t.astype(jnp.bfloat16)
                wp[rs, c:c + LANES] = w.astype(jnp.bfloat16)
                up[rs, c + band:c + band + LANES] = tt.astype(jnp.bfloat16)
                wp[rs, c + band:c + band + LANES] = wt.astype(jnp.bfloat16)
        folds = [q[0:8] + q[8:16] for q in tots]
        eacc[x] = eacc[x] + sum(folds)
        for n in range(nb):
            eacc[s0 + n] = eacc[s0 + n] + folds[n] + jnp.where(in_band(n), folds[nb], 0.0)

    vside = vmat[:, LANES:WIDE]
    vmix = jnp.ones((rows, LANES), jnp.float32)
    for n in range(nb):
        vmix = jnp.where(in_band(n), vside if n == 0 else pltpu.roll(vside, n * extra, 1), vmix)
    vrest[...] = vmix
    ktp[...] = jnp.zeros_like(ktp)

    ring = nb // 2
    work([(own0 + i, own0 + i) for i in range(nb)]
         + [(own0 + i, own0 + (i + d) % nb) for d in range(1, ring + 1) for i in range(nb)], diag=range(nb))

    to_s[0].wait_recv()
    unpack(3, sib0)
    to_s[1].wait_recv()

    def sib_pair(i, d):
        j = lax.rem(i + d, nb)
        return own0 + jnp.where(core == 0, i, j), sib0 + jnp.where(core == 0, j, i)

    shift = jnp.where(core == 0, 0, ring + 1)
    cut = (nb + 1) // 2
    rest = [(jnp.where(core == 0, i, jnp.minimum(cut + i, nb - 1)), ring) for i in range(cut)]
    work([sib_pair(i, d + shift) for d in range(ring) for i in range(nb)] + [sib_pair(i, d) for i, d in rest],
         weight={ring * nb + cut - 1: jnp.where(core == 0, 1.0, 0.0)})

    def arrive(late, s):
        remote(cols(own0), cols(e0 + late * nb + s), nbr_send.at[0, s], nbr_sem.at[late, s], n_dst).wait_recv()

    def arrive_rest(late):
        remote(pack.at[0], pack.at[1 + late], nbr_send.at[0, nb], nbr_sem.at[late, nb], n_dst).wait_recv()
        unpack(1 + late, e0 + late * nb)

    def with_own(slot):
        return [(own0 + i, slot) for i in range(nb)]

    head = nb // 2
    pack_rows(0, own0)
    arrive_rest(0)
    for s in range(head):
        arrive(0, s)
    work([q for s in range(head) for q in with_own(e0 + s)])
    arrive(0, head)
    work(with_own(e0 + head))
    launch(to_n[0:nb], jnp.logical_not(n_early))
    launch(to_p[0:nb], jnp.logical_not(p_early))

    for s in range(head + 1, nb):
        arrive(0, s)
    work([q for s in range(head + 1, nb) for q in with_own(e0 + s)])
    arrive_rest(1)

    pack_rows(1, e0)

    def late_step(j, _):
        arrive(1, j)
        late_group(0, l0 + j, own0)
        late_group(1, l0 + j, e0)
        dacc[:, 0:rows] = dacc[:, 0:rows] + lax.dot_general(up[...], wp[...], (((1,), (1,)), ((), ())),
                                                            preferred_element_type=jnp.float32)
        return 0

    lax.fori_loop(0, nb, late_step, 0)

    stack = 32
    part[0:nv, :] = dacc[0:nv, 0:LANES]
    rest = dacc[:, LANES:WIDE]
    mix = rest[0:stack]
    for g in range(1, rows // stack):
        mix = mix + pltpu.roll(rest[g * stack:(g + 1) * stack], g * extra, 1)
    part[nv:nv + stack, :] = mix

    cut_rows = red_ref.shape[0] // n_dev
    reds, gats, es = [], [], []
    order = sorted(range(1, n_dev), key=lambda r: -min(r, n_dev - r))
    for r in order:
        dst = lax.rem(me + r, n_dev)
        reds.append(remote(part.at[pl.ds(dst * cut_rows, cut_rows)], rbuf.at[r - 1], red_send.at[r - 1], red_recv.at[r - 1], dst))
        reds[-1].start()

    lane1 = lax.broadcasted_iota(jnp.int32, (1, LANES), 1)
    erow = jnp.zeros((1, LANES), jnp.float32)
    for kind, dev in enumerate((me, sib, e_src, l_src)):
        for s in range(nb):
            e_val = jnp.sum(jnp.sum(eacc[kind * nb + s], axis=0, keepdims=True), axis=1, keepdims=True)
            erow = erow + jnp.where(lane1 == dev * nb + s, e_val, 0.0)
    elocal[...] = erow
    for r in range(1, n_dev):
        es.append(remote(elocal, ebuf.at[r - 1], e_send.at[r - 1], e_recv.at[r - 1], lax.rem(me + r, n_dev)))
        es[-1].start()

    mine = pl.ds(me * cut_rows, cut_rows)
    for c in reds:
        c.wait_recv()
    total = part[mine, :]
    for r in range(1, n_dev):
        total = total + rbuf[r - 1]
    red_ref[mine, :] = total
    for r in order:
        dst = lax.rem(me + r, n_dev)
        gats.append(remote(red_ref.at[mine], red_ref.at[mine], gat_send.at[r - 1], gat_recv.at[r - 1], dst))
        gats[-1].start()
    for c in es:
        c.wait_recv()
    place = lax.rem(me, n_dev)
    e_all = jnp.zeros((1, LANES), jnp.float32)
    for d in range(n_dev):
        took = elocal[...]
        for r in range(1, n_dev):
            took = jnp.where(lax.rem(place + n_dev - r, n_dev) == d, ebuf[r - 1], took)
        e_all = e_all + took
    e_ref[0:1, :] = pltpu.roll(jnp.broadcast_to(e_all, (8, LANES)), lax.rem(LANES - me * nb, LANES), 1)[0:1]
    e_ref[1:2, :] = jnp.broadcast_to(jnp.sum(e_all, axis=1, keepdims=True), (1, LANES))
    for r in range(1, n_dev):
        src = lax.rem(me + n_dev - r, n_dev)
        remote(red_ref.at[mine], red_ref.at[pl.ds(src * cut_rows, cut_rows)], gat_send.at[r - 1], gat_recv.at[r - 1], src).wait_recv()
    for c in to_n + to_p + to_s + reds + gats + es:
        c.wait_send()


def finish(nb, nv, red_ref, e_ref, dens_ref, epair_ref, energy_ref):
    extra, stack = nv - LANES, 32
    dens_ref[:, 0:LANES] = red_ref[0:nv, :]
    mix = red_ref[nv:nv + stack, :]
    for g in range(-(-nv // stack)):
        n = min(stack, nv - g * stack)
        side = mix if g == 0 else pltpu.roll(mix, LANES - g * extra, 1)
        dens_ref[g * stack:g * stack + n, LANES:nv] = side[0:n, 0:extra]
    epair_ref[...] = e_ref[0:1, 0:nb]
    energy_ref[...] = e_ref[1:2, 0:1]


def solution(mesh):
    n_dev = mesh.shape['occ']

    def per_device(b_blk, eps_occ, eps_vir):
        nq, nb, nv = b_blk.shape
        rows = (nv + 15) // 16 * 16
        n_cut = -(-(nv + 32) // n_dev)
        cut_rows = (n_cut + 7) // 8 * 8
        deep = (nq + LANES - 1) // LANES * LANES
        most = 3 * nb
        by_orb = jnp.transpose(b_blk, (1, 2, 0))
        vmem = pltpu.VMEM
        dma = pltpu.SemaphoreType.DMA
        f32, bf16 = jnp.float32, jnp.bfloat16
        anyspace = pl.BlockSpec(memory_space=pl.ANY)
        in_vmem = pl.BlockSpec(memory_space=vmem)
        red, e_rows = pl.pallas_call(
            functools.partial(kernel, n_dev, nb, nv, nq),
            out_shape=(jax.ShapeDtypeStruct((n_dev * cut_rows, LANES), f32), jax.ShapeDtypeStruct((8, LANES), f32)),
            in_specs=[anyspace] * 3,
            out_specs=(in_vmem,) * 2,
            scratch_shapes=[
                vmem((4 * nb, rows, deep), bf16),
                vmem((nb, nv, nq % LANES), bf16),
                vmem((4, nb, rows // (LANES // (nq % LANES)), LANES), bf16),
                pltpu.SMEM((nb * n_dev,), f32),
                vmem((1, nv), f32),
                vmem((most, rows, WIDE), f32),
                vmem((most, rows, WIDE), f32),
                vmem((rows, 2 * most * WIDE), bf16),
                vmem((2 * most * WIDE, WIDE), bf16),
                vmem((rows, WIDE), f32),
                vmem((4 * nb, 8, LANES), f32),
                vmem((rows, WIDE), f32),
                vmem((n_dev * cut_rows, LANES), f32),
                vmem((n_dev - 1, cut_rows, LANES), f32),
                vmem((n_dev - 1, 1, LANES), f32),
                vmem((1, LANES), f32),
                vmem((2, deep, (nb + 1) * LANES), bf16),
                vmem((2, rows, (nb + 1) * LANES), f32),
                vmem((2, rows, (nb + 1) * LANES), f32),
                vmem((rows, 4 * (nb + 1) * LANES), bf16),
                vmem((rows, 4 * (nb + 1) * LANES), bf16),
                vmem((rows, LANES), f32),
                dma((4,)), dma((2, 2)), dma((2, nb + 1)), dma((2, nb + 1)),
                dma((n_dev - 1,)), dma((n_dev - 1,)), dma((n_dev - 1,)), dma((n_dev - 1,)),
                dma((n_dev - 1,)), dma((n_dev - 1,)),
            ],
            compiler_params=pltpu.CompilerParams(collective_id=0, has_side_effects=True),
        )(by_orb, eps_occ, eps_vir.reshape(1, nv))
        dens, e_pair, energy = pl.pallas_call(
            functools.partial(finish, nb, nv),
            out_shape=(jax.ShapeDtypeStruct((nv, nv), f32), jax.ShapeDtypeStruct((1, nb), f32), jax.ShapeDtypeStruct((1, 1), f32)),
            in_specs=[in_vmem] * 2,
            out_specs=(in_vmem,) * 3,
        )(red, e_rows)
        return e_pair.reshape(nb), energy.reshape(1), dens

    return jax.shard_map(per_device, mesh=mesh, in_specs=(P(None, ('mol', 'occ'), None), P('mol'), P('mol')),
                         out_specs=(P(('mol', 'occ')), P('mol'), P('mol', None)), check_vma=False)
```

```python
import functools

import jax
import jax.numpy as jnp
from jax import lax
from jax.experimental import pallas as pl
from jax.experimental.pallas import tpu as pltpu
from jax.sharding import PartitionSpec as P

MESH_ID = pl.DeviceIdType.MESH
CORES = 2
LANES = 128
WIDE = 2 * LANES


def flip(bit, by):
    return lax.rem(bit + by, CORES)


def remote(src, dst, send, recv, dev):
    return pltpu.make_async_remote_copy(src_ref=src, dst_ref=dst, send_sem=send, recv_sem=recv,
                                        device_id={'occ': dev}, device_id_type=MESH_ID)


def kernel(n_dev, nb, nv, nq, b_ref, eo_ref, ev_ref, red_ref, e_ref,
           blk, rem, pack, eo, ev, kbuf, ktbuf, ucat, wcat, vmat, eacc, dacc, part, rbuf, hbuf, ebuf, elocal,
           ypt, kp, ktp, up, wp, vrest,
           load_sem, sib_sem, nbr_send, nbr_sem, red_send, red_recv, gat_send, gat_recv, e_send, e_recv):
    rows = vmat.shape[0]
    main = nq // LANES * LANES
    deep = blk.shape[2]
    tail = nq - main
    packed = pack.shape[2]
    n_chip = n_dev // CORES
    me = lax.axis_index('occ')
    chip, core = me // CORES, lax.rem(me, CORES)
    nxt, prv = lax.rem(chip + 1, n_chip), lax.rem(chip + n_chip - 1, n_chip)
    first = lambda c: jnp.where(c == 0, 1, 0)
    n_src = nxt * CORES + flip(core, first(chip))
    p_src = prv * CORES + flip(core, 1 + first(prv))
    n_dst = prv * CORES + flip(core, first(prv))
    p_dst = nxt * CORES + flip(core, 1 + first(chip))
    sib = chip * CORES + flip(core, 1)
    own0, sib0, e0, l0 = 0, nb, 2 * nb, 3 * nb
    n_early = core == 0
    p_early = core == flip(first(chip), first(nxt))
    got_n_early = flip(core, first(chip)) == 0
    e_src = jnp.where(got_n_early, n_src, p_src)
    l_src = jnp.where(got_n_early, p_src, n_src)

    barrier = pltpu.get_barrier_semaphore()
    for r in range(1, n_dev):
        pl.semaphore_signal(barrier, inc=1, device_id={'occ': lax.rem(me + r, n_dev)}, device_id_type=MESH_ID)
    loads = [pltpu.make_async_copy(b_ref.at[:, :, main:nq], rem, load_sem.at[0]),
             pltpu.make_async_copy(b_ref.at[:, :, 0:main], blk.at[pl.ds(own0, nb), 0:nv, 0:main], load_sem.at[1]),
             pltpu.make_async_copy(eo_ref, eo, load_sem.at[2]),
             pltpu.make_async_copy(ev_ref, ev, load_sem.at[3])]
    for c in loads:
        c.start()

    for s in range(4 * nb):
        blk[s, nv:rows, :] = jnp.zeros((rows - nv, blk.shape[2]), jnp.bfloat16)
    for g in range(kbuf.shape[0]):
        kbuf[g, :, LANES:WIDE] = jnp.zeros((rows, LANES), jnp.float32)
        ktbuf[g, :, LANES:WIDE] = jnp.zeros((rows, LANES), jnp.float32)
    for g in range(wcat.shape[0] // WIDE):
        wcat[g * WIDE + rows:(g + 1) * WIDE, :] = jnp.zeros((WIDE - rows, WIDE), jnp.bfloat16)
    eacc[...] = jnp.zeros_like(eacc)
    dacc[...] = jnp.zeros_like(dacc)
    part[...] = jnp.zeros_like(part)

    lane = lax.broadcasted_iota(jnp.int32, (packed, LANES), 1)
    groups = LANES // tail
    loads[0].wait()
    for s in range(nb):
        own_tail = jnp.concatenate([rem[s].astype(jnp.float32), jnp.zeros((nv, LANES - tail), jnp.float32)], axis=1)
        blk[own0 + s, 0:nv, main:main + LANES] = own_tail.astype(jnp.bfloat16)
        filled = jnp.concatenate([own_tail, jnp.zeros((groups * packed - nv, LANES), jnp.float32)], axis=0)
        mix = filled[0:packed]
        for g in range(1, groups):
            mix = mix + pltpu.roll(filled[g * packed:(g + 1) * packed], g * tail, 1)
        pack[0, s] = mix.astype(jnp.bfloat16)
    loads[2].wait()
    loads[3].wait()
    vrow = jnp.broadcast_to(ev[...], (nv, nv))
    vmat[...] = jnp.ones_like(vmat)
    vmat[0:nv, 0:nv] = vrow + vrow.T
    loads[1].wait()
    pl.semaphore_wait(barrier, n_dev - 1)

    def cols(slot):
        return blk.at[slot, 0:nv, 0:main]

    def flow(which, early, dst):
        late = jnp.where(early, 0, 1)
        return ([remote(cols(own0 + s), cols(e0 + late * nb + s), nbr_send.at[which, s], nbr_sem.at[late, s], dst)
                 for s in range(nb)]
                + [remote(pack.at[0], pack.at[1 + late], nbr_send.at[which, nb], nbr_sem.at[late, nb], dst)])

    to_n, to_p = flow(0, n_early, n_dst), flow(1, p_early, p_dst)
    to_s = [remote(pack.at[0], pack.at[3], sib_sem.at[0, 0], sib_sem.at[1, 0], sib),
            remote(blk.at[pl.ds(own0, nb), 0:nv, 0:main], blk.at[pl.ds(sib0, nb), 0:nv, 0:main],
                   sib_sem.at[0, 1], sib_sem.at[1, 1], sib)]

    def launch(copies, when):
        @pl.when(when)
        def _():
            for c in copies:
                c.start()

    to_n[nb].start()
    to_p[nb].start()
    launch(to_n[0:nb], n_early)
    launch(to_p[0:nb], p_early)
    for c in to_s:
        c.start()

    def unpack(which, slot0):
        for s in range(nb):
            mix = pack[which, s].astype(jnp.float32)
            parts = [mix] + [pltpu.roll(mix, LANES - g * tail, 1) for g in range(1, groups)]
            full = jnp.concatenate([jnp.where(lane < tail, q, 0.0) for q in parts], axis=0)
            blk[slot0 + s, :, main:main + LANES] = full.astype(jnp.bfloat16)

    def orb_energy(slot):
        if isinstance(slot, int):
            dev = (me, sib, e_src, l_src)[slot // nb]
            return eo[dev * nb + slot % nb]
        kind, off = slot // nb, lax.rem(slot, nb)
        dev = jnp.where(kind == 0, me, jnp.where(kind == 1, sib, jnp.where(kind == 2, e_src, l_src)))
        return eo[dev * nb + off]

    def work(pairs, diag=(), weight=None):
        c0 = 0
        for g, (x, y) in enumerate(pairs):
            k_pair = lax.dot_general(blk[x], blk[y], (((1,), (1,)), ((), ())), preferred_element_type=jnp.float32)
            kbuf[g, :, 0:rows] = k_pair
            ktbuf[g, :, 0:rows] = k_pair.T
            e_sum = orb_energy(x) + orb_energy(y)
            tot = jnp.zeros((16, WIDE), jnp.float32)
            for r0 in range(0, rows, 16):
                rs = pl.ds(r0, 16)
                k, kt = kbuf[g, rs, :], ktbuf[g, rs, :]
                rec = 1.0 / (e_sum - vmat[rs, :])
                if weight is not None and g in weight:
                    rec = rec * weight[g]
                t, tt = k * rec, kt * rec
                w, wt = (t + t) - tt, (tt + tt) - t
                tot = tot + k * w
                ucat[rs, c0:c0 + WIDE] = t.astype(jnp.bfloat16)
                wcat[pl.ds(c0 + r0, 16), :] = wt.astype(jnp.bfloat16)
                if g not in diag:
                    c1 = c0 + WIDE
                    ucat[rs, c1:c1 + WIDE] = tt.astype(jnp.bfloat16)
                    wcat[pl.ds(c1 + r0, 16), :] = w.astype(jnp.bfloat16)
            c0 += WIDE if g in diag else 2 * WIDE
            fold = tot[0:8, 0:LANES] + tot[8:16, 0:LANES] + tot[0:8, LANES:WIDE] + tot[8:16, LANES:WIDE]
            eacc[x] = eacc[x] + fold
            if g not in diag:
                eacc[y] = eacc[y] + fold
        dacc[...] = dacc[...] + jnp.dot(ucat[:, 0:c0], wcat[0:c0, :], preferred_element_type=jnp.float32)

    extra = nv - LANES
    tiles = nb + 1
    band = tiles * LANES
    side = nb * LANES
    lane128 = lax.broadcasted_iota(jnp.int32, (1, LANES), 1)

    def in_band(j):
        return (lane128 >= j * extra) & (lane128 < (j + 1) * extra)

    def pack_rows(which, s0):
        for n in range(nb):
            ypt[which, :, n * LANES:(n + 1) * LANES] = blk[s0 + n, 0:LANES, :].astype(jnp.float32).T.astype(jnp.bfloat16)
        rests = [blk[s0 + n, LANES:rows, :].astype(jnp.float32)[0:extra] for n in range(nb)]
        rests.append(jnp.zeros((LANES - nb * extra, deep), jnp.float32))
        ypt[which, :, side:band] = jnp.concatenate(rests, axis=0).T.astype(jnp.bfloat16)

    def late_group(g, x, s0):
        kp[g] = jnp.dot(blk[x], ypt[g], preferred_element_type=jnp.float32)
        side_t = kp[g, 0:LANES, side:band].T
        for n in range(nb):
            at = pl.ds(n * LANES, LANES)
            ktp[g, 0:LANES, at] = kp[g, 0:LANES, at].T
            ktp[g, LANES:nv, at] = side_t[n * extra:(n + 1) * extra]
        low = [kp[g, LANES:nv, n * LANES:(n + 1) * LANES] for n in range(nb)]
        low.append(jnp.zeros((LANES - nb * extra, LANES), jnp.float32))
        ktp[g, 0:LANES, side:band] = jnp.concatenate(low, axis=0).T
        corner = kp[g, LANES:nv, side:band]
        corner_t = jnp.concatenate([corner, jnp.zeros((LANES - extra, LANES), jnp.float32)], axis=0).T
        spread = corner_t[0:extra]
        for n in range(1, nb):
            spread = spread + pltpu.roll(corner_t[n * extra:(n + 1) * extra], n * extra, 1)
        ktp[g, LANES:nv, side:band] = spread
        e_x = orb_energy(x)
        e_sums = [e_x + orb_energy(s0 + n) for n in range(nb)]
        e_rest = jnp.full((1, LANES), e_sums[nb - 1], jnp.float32)
        for n in range(nb - 1):
            e_rest = jnp.where(in_band(n), e_sums[n], e_rest)
        tots = [jnp.zeros((16, LANES), jnp.float32) for _ in range(tiles)]
        c0 = 2 * g * band
        for r0 in range(0, rows, 16):
            rs = pl.ds(r0, 16)
            for n in range(tiles):
                k, kt = kp[g, rs, n * LANES:(n + 1) * LANES], ktp[g, rs, n * LANES:(n + 1) * LANES]
                den = e_rest - vrest[rs, :] if n == nb else e_sums[n] - vmat[rs, 0:LANES]
                rec = 1.0 / den
                t, tt = k * rec, kt * rec
                w, wt = (t + t) - tt, (tt + tt) - t
                tots[n] = tots[n] + k * w
                c = c0 + n * LANES
                up[rs, c:c + LANES] = t.astype(jnp.bfloat16)
                wp[rs, c:c + LANES] = w.astype(jnp.bfloat16)
                up[rs, c + band:c + band + LANES] = tt.astype(jnp.bfloat16)
                wp[rs, c + band:c + band + LANES] = wt.astype(jnp.bfloat16)
        folds = [q[0:8] + q[8:16] for q in tots]
        eacc[x] = eacc[x] + sum(folds)
        for n in range(nb):
            eacc[s0 + n] = eacc[s0 + n] + folds[n] + jnp.where(in_band(n), folds[nb], 0.0)

    vside = vmat[:, LANES:WIDE]
    vmix = jnp.ones((rows, LANES), jnp.float32)
    for n in range(nb):
        vmix = jnp.where(in_band(n), vside if n == 0 else pltpu.roll(vside, n * extra, 1), vmix)
    vrest[...] = vmix
    ktp[...] = jnp.zeros_like(ktp)

    ring = nb // 2
    work([(own0 + i, own0 + i) for i in range(nb)]
         + [(own0 + i, own0 + (i + d) % nb) for d in range(1, ring + 1) for i in range(nb)], diag=range(nb))

    to_s[0].wait_recv()
    unpack(3, sib0)
    to_s[1].wait_recv()

    def sib_pair(i, d):
        j = lax.rem(i + d, nb)
        return own0 + jnp.where(core == 0, i, j), sib0 + jnp.where(core == 0, j, i)

    shift = jnp.where(core == 0, 0, ring + 1)
    cut = (nb + 1) // 2
    rest = [(jnp.where(core == 0, i, jnp.minimum(cut + i, nb - 1)), ring) for i in range(cut)]
    work([sib_pair(i, d + shift) for d in range(ring) for i in range(nb)] + [sib_pair(i, d) for i, d in rest],
         weight={ring * nb + cut - 1: jnp.where(core == 0, 1.0, 0.0)})

    def arrive(late, s):
        remote(cols(own0), cols(e0 + late * nb + s), nbr_send.at[0, s], nbr_sem.at[late, s], n_dst).wait_recv()

    def arrive_rest(late):
        remote(pack.at[0], pack.at[1 + late], nbr_send.at[0, nb], nbr_sem.at[late, nb], n_dst).wait_recv()
        unpack(1 + late, e0 + late * nb)

    def with_own(slot):
        return [(own0 + i, slot) for i in range(nb)]

    head = nb // 2
    pack_rows(0, own0)
    arrive_rest(0)
    for s in range(head):
        arrive(0, s)
    work([q for s in range(head) for q in with_own(e0 + s)])
    arrive(0, head)
    work(with_own(e0 + head))
    launch(to_n[0:nb], jnp.logical_not(n_early))
    launch(to_p[0:nb], jnp.logical_not(p_early))

    for s in range(head + 1, nb):
        arrive(0, s)
    work([q for s in range(head + 1, nb) for q in with_own(e0 + s)])
    arrive_rest(1)

    pack_rows(1, e0)

    def late_step(j, _):
        arrive(1, j)
        late_group(0, l0 + j, own0)
        late_group(1, l0 + j, e0)
        dacc[:, 0:rows] = dacc[:, 0:rows] + lax.dot_general(up[...], wp[...], (((1,), (1,)), ((), ())),
                                                            preferred_element_type=jnp.float32)
        return 0

    lax.fori_loop(0, nb, late_step, 0)

    stack = 32
    part[0:nv, :] = dacc[0:nv, 0:LANES]
    rest = dacc[:, LANES:WIDE]
    mix = rest[0:stack]
    for g in range(1, rows // stack):
        mix = mix + pltpu.roll(rest[g * stack:(g + 1) * stack], g * extra, 1)
    part[nv:nv + stack, :] = mix

    half = red_ref.shape[0] // CORES
    mine, other = pl.ds(core * half, half), pl.ds(flip(core, 1) * half, half)
    swap = remote(part.at[other], rbuf, red_send.at[0], red_recv.at[0], sib)
    swap.start()
    es, sums = [], []
    hops = sorted(range(1, n_chip), key=lambda r: -min(r, n_chip - r))
    swap.wait_recv()
    hbuf[chip] = part[mine, :] + rbuf[...]
    for r in hops:
        dst = lax.rem(chip + r, n_chip) * CORES + core
        sums.append(remote(hbuf.at[chip], hbuf.at[chip], red_send.at[r], red_recv.at[r], dst))
        sums[-1].start()

    lane1 = lax.broadcasted_iota(jnp.int32, (1, LANES), 1)
    erow = jnp.zeros((1, LANES), jnp.float32)
    for kind, dev in enumerate((me, sib, e_src, l_src)):
        for s in range(nb):
            e_val = jnp.sum(jnp.sum(eacc[kind * nb + s], axis=0, keepdims=True), axis=1, keepdims=True)
            erow = erow + jnp.where(lane1 == dev * nb + s, e_val, 0.0)
    elocal[...] = erow
    for r in range(1, n_dev):
        es.append(remote(elocal, ebuf.at[r - 1], e_send.at[r - 1], e_recv.at[r - 1], lax.rem(me + r, n_dev)))
        es[-1].start()

    for r in range(1, n_chip):
        src = lax.rem(chip + n_chip - r, n_chip)
        remote(hbuf.at[chip], hbuf.at[src], red_send.at[r], red_recv.at[r], src * CORES + core).wait_recv()
    total = hbuf[0]
    for r in range(1, n_chip):
        total = total + hbuf[r]
    red_ref[mine, :] = total
    back = remote(red_ref.at[mine], red_ref.at[mine], gat_send, gat_recv, sib)
    back.start()
    for c in es:
        c.wait_recv()
    place = lax.rem(me, n_dev)
    e_all = jnp.zeros((1, LANES), jnp.float32)
    for d in range(n_dev):
        took = elocal[...]
        for r in range(1, n_dev):
            took = jnp.where(lax.rem(place + n_dev - r, n_dev) == d, ebuf[r - 1], took)
        e_all = e_all + took
    e_ref[0:1, :] = pltpu.roll(jnp.broadcast_to(e_all, (8, LANES)), lax.rem(LANES - me * nb, LANES), 1)[0:1]
    e_ref[1:2, :] = jnp.broadcast_to(jnp.sum(e_all, axis=1, keepdims=True), (1, LANES))
    remote(red_ref.at[mine], red_ref.at[other], gat_send, gat_recv, sib).wait_recv()
    for c in to_n + to_p + to_s + sums + es + [swap, back]:
        c.wait_send()


def finish(nb, nv, red_ref, e_ref, dens_ref, epair_ref, energy_ref):
    extra, stack = nv - LANES, 32
    dens_ref[:, 0:LANES] = red_ref[0:nv, :]
    mix = red_ref[nv:nv + stack, :]
    for g in range(-(-nv // stack)):
        n = min(stack, nv - g * stack)
        side = mix if g == 0 else pltpu.roll(mix, LANES - g * extra, 1)
        dens_ref[g * stack:g * stack + n, LANES:nv] = side[0:n, 0:extra]
    epair_ref[...] = e_ref[0:1, 0:nb]
    energy_ref[...] = e_ref[1:2, 0:1]


def solution(mesh):
    n_dev = mesh.shape['occ']

    def per_device(b_blk, eps_occ, eps_vir):
        nq, nb, nv = b_blk.shape
        rows = (nv + 15) // 16 * 16
        n_cut = -(-(nv + 32) // n_dev)
        cut_rows = (n_cut + 7) // 8 * 8
        deep = (nq + LANES - 1) // LANES * LANES
        most = 3 * nb
        by_orb = jnp.transpose(b_blk, (1, 2, 0))
        vmem = pltpu.VMEM
        dma = pltpu.SemaphoreType.DMA
        f32, bf16 = jnp.float32, jnp.bfloat16
        anyspace = pl.BlockSpec(memory_space=pl.ANY)
        in_vmem = pl.BlockSpec(memory_space=vmem)
        red, e_rows = pl.pallas_call(
            functools.partial(kernel, n_dev, nb, nv, nq),
            out_shape=(jax.ShapeDtypeStruct((n_dev * cut_rows, LANES), f32), jax.ShapeDtypeStruct((8, LANES), f32)),
            in_specs=[anyspace] * 3,
            out_specs=(in_vmem,) * 2,
            scratch_shapes=[
                vmem((4 * nb, rows, deep), bf16),
                vmem((nb, nv, nq % LANES), bf16),
                vmem((4, nb, rows // (LANES // (nq % LANES)), LANES), bf16),
                pltpu.SMEM((nb * n_dev,), f32),
                vmem((1, nv), f32),
                vmem((most, rows, WIDE), f32),
                vmem((most, rows, WIDE), f32),
                vmem((rows, 2 * most * WIDE), bf16),
                vmem((2 * most * WIDE, WIDE), bf16),
                vmem((rows, WIDE), f32),
                vmem((4 * nb, 8, LANES), f32),
                vmem((rows, WIDE), f32),
                vmem((n_dev * cut_rows, LANES), f32),
                vmem((n_dev * cut_rows // CORES, LANES), f32),
                vmem((n_dev // CORES, n_dev * cut_rows // CORES, LANES), f32),
                vmem((n_dev - 1, 1, LANES), f32),
                vmem((1, LANES), f32),
                vmem((2, deep, (nb + 1) * LANES), bf16),
                vmem((2, rows, (nb + 1) * LANES), f32),
                vmem((2, rows, (nb + 1) * LANES), f32),
                vmem((rows, 4 * (nb + 1) * LANES), bf16),
                vmem((rows, 4 * (nb + 1) * LANES), bf16),
                vmem((rows, LANES), f32),
                dma((4,)), dma((2, 2)), dma((2, nb + 1)), dma((2, nb + 1)),
                dma((n_dev // CORES,)), dma((n_dev // CORES,)), dma, dma, dma((n_dev - 1,)), dma((n_dev - 1,)),
            ],
            compiler_params=pltpu.CompilerParams(collective_id=0, has_side_effects=True),
        )(by_orb, eps_occ, eps_vir.reshape(1, nv))
        dens, e_pair, energy = pl.pallas_call(
            functools.partial(finish, nb, nv),
            out_shape=(jax.ShapeDtypeStruct((nv, nv), f32), jax.ShapeDtypeStruct((1, nb), f32), jax.ShapeDtypeStruct((1, 1), f32)),
            in_specs=[in_vmem] * 2,
            out_specs=(in_vmem,) * 3,
        )(red, e_rows)
        return e_pair.reshape(nb), energy.reshape(1), dens

    return jax.shard_map(per_device, mesh=mesh, in_specs=(P(None, ('mol', 'occ'), None), P('mol'), P('mol')),
                         out_specs=(P(('mol', 'occ')), P('mol'), P('mol', None)), check_vma=False)
```

```python
import functools

import jax
import jax.numpy as jnp
from jax import lax
from jax.experimental import pallas as pl
from jax.experimental.pallas import tpu as pltpu
from jax.sharding import PartitionSpec as P

MESH_ID = pl.DeviceIdType.MESH
CORES = 2
LANES = 128
WIDE = 2 * LANES


def flip(bit, by):
    return lax.rem(bit + by, CORES)


def remote(src, dst, send, recv, dev):
    return pltpu.make_async_remote_copy(src_ref=src, dst_ref=dst, send_sem=send, recv_sem=recv,
                                        device_id={'occ': dev}, device_id_type=MESH_ID)


def kernel(n_dev, nb, nv, nq, b_ref, eo_ref, ev_ref, red_ref, e_ref,
           blk, rem, pack, eo, ev, kbuf, ktbuf, ucat, wcat, vmat, eacc, dacc, part, rbuf, hbuf, ebuf, elocal,
           ypt, kp, ktp, up, wp, vrest,
           load_sem, sib_sem, nbr_send, nbr_sem, red_send, red_recv, gat_send, gat_recv, e_send, e_recv):
    rows = vmat.shape[0]
    main = nq // LANES * LANES
    deep = blk.shape[2]
    tail = nq - main
    packed = pack.shape[2]
    n_chip = n_dev // CORES
    me = lax.axis_index('occ')
    chip, core = me // CORES, lax.rem(me, CORES)
    nxt, prv = lax.rem(chip + 1, n_chip), lax.rem(chip + n_chip - 1, n_chip)
    first = lambda c: jnp.where(c == 0, 1, 0)
    n_src = nxt * CORES + flip(core, first(chip))
    p_src = prv * CORES + flip(core, 1 + first(prv))
    n_dst = prv * CORES + flip(core, first(prv))
    p_dst = nxt * CORES + flip(core, 1 + first(chip))
    sib = chip * CORES + flip(core, 1)
    own0, sib0, e0, l0 = 0, nb, 2 * nb, 3 * nb
    n_early = core == 0
    p_early = core == flip(first(chip), first(nxt))
    got_n_early = flip(core, first(chip)) == 0
    e_src = jnp.where(got_n_early, n_src, p_src)
    l_src = jnp.where(got_n_early, p_src, n_src)

    barrier = pltpu.get_barrier_semaphore()
    for r in range(1, n_dev):
        pl.semaphore_signal(barrier, inc=1, device_id={'occ': lax.rem(me + r, n_dev)}, device_id_type=MESH_ID)
    loads = [pltpu.make_async_copy(b_ref.at[:, :, main:nq], rem, load_sem.at[0]),
             pltpu.make_async_copy(b_ref.at[:, :, 0:main], blk.at[pl.ds(own0, nb), 0:nv, 0:main], load_sem.at[1]),
             pltpu.make_async_copy(eo_ref, eo, load_sem.at[2]),
             pltpu.make_async_copy(ev_ref, ev, load_sem.at[3])]
    for c in loads:
        c.start()

    for s in range(4 * nb):
        blk[s, nv:rows, :] = jnp.zeros((rows - nv, blk.shape[2]), jnp.bfloat16)
    for g in range(kbuf.shape[0]):
        kbuf[g, :, LANES:WIDE] = jnp.zeros((rows, LANES), jnp.float32)
        ktbuf[g, :, LANES:WIDE] = jnp.zeros((rows, LANES), jnp.float32)
    for g in range(wcat.shape[0] // WIDE):
        wcat[g * WIDE + rows:(g + 1) * WIDE, :] = jnp.zeros((WIDE - rows, WIDE), jnp.bfloat16)
    eacc[...] = jnp.zeros_like(eacc)
    dacc[...] = jnp.zeros_like(dacc)
    part[...] = jnp.zeros_like(part)

    lane = lax.broadcasted_iota(jnp.int32, (packed, LANES), 1)
    groups = LANES // tail
    loads[0].wait()
    for s in range(nb):
        own_tail = jnp.concatenate([rem[s].astype(jnp.float32), jnp.zeros((nv, LANES - tail), jnp.float32)], axis=1)
        blk[own0 + s, 0:nv, main:main + LANES] = own_tail.astype(jnp.bfloat16)
        filled = jnp.concatenate([own_tail, jnp.zeros((groups * packed - nv, LANES), jnp.float32)], axis=0)
        mix = filled[0:packed]
        for g in range(1, groups):
            mix = mix + pltpu.roll(filled[g * packed:(g + 1) * packed], g * tail, 1)
        pack[0, s] = mix.astype(jnp.bfloat16)
    loads[2].wait()
    loads[3].wait()
    vrow = jnp.broadcast_to(ev[...], (nv, nv))
    vmat[...] = jnp.ones_like(vmat)
    vmat[0:nv, 0:nv] = vrow + vrow.T
    loads[1].wait()
    pl.semaphore_wait(barrier, n_dev - 1)

    def cols(slot):
        return blk.at[slot, 0:nv, 0:main]

    def flow(which, early, dst):
        late = jnp.where(early, 0, 1)
        return ([remote(cols(own0 + s), cols(e0 + late * nb + s), nbr_send.at[which, s], nbr_sem.at[late, s], dst)
                 for s in range(nb)]
                + [remote(pack.at[0], pack.at[1 + late], nbr_send.at[which, nb], nbr_sem.at[late, nb], dst)])

    to_n, to_p = flow(0, n_early, n_dst), flow(1, p_early, p_dst)
    to_s = [remote(pack.at[0], pack.at[3], sib_sem.at[0, 0], sib_sem.at[1, 0], sib),
            remote(blk.at[pl.ds(own0, nb), 0:nv, 0:main], blk.at[pl.ds(sib0, nb), 0:nv, 0:main],
                   sib_sem.at[0, 1], sib_sem.at[1, 1], sib)]

    def launch(copies, when):
        @pl.when(when)
        def _():
            for c in copies:
                c.start()

    to_n[nb].start()
    to_p[nb].start()
    launch(to_n[0:nb], n_early)
    launch(to_p[0:nb], p_early)
    for c in to_s:
        c.start()

    def unpack(which, slot0):
        for s in range(nb):
            mix = pack[which, s].astype(jnp.float32)
            parts = [mix] + [pltpu.roll(mix, LANES - g * tail, 1) for g in range(1, groups)]
            full = jnp.concatenate([jnp.where(lane < tail, q, 0.0) for q in parts], axis=0)
            blk[slot0 + s, :, main:main + LANES] = full.astype(jnp.bfloat16)

    def orb_energy(slot):
        if isinstance(slot, int):
            dev = (me, sib, e_src, l_src)[slot // nb]
            return eo[dev * nb + slot % nb]
        kind, off = slot // nb, lax.rem(slot, nb)
        dev = jnp.where(kind == 0, me, jnp.where(kind == 1, sib, jnp.where(kind == 2, e_src, l_src)))
        return eo[dev * nb + off]

    def work(pairs, diag=(), weight=None):
        c0 = 0
        for g, (x, y) in enumerate(pairs):
            k_pair = lax.dot_general(blk[x], blk[y], (((1,), (1,)), ((), ())), preferred_element_type=jnp.float32)
            kbuf[g, :, 0:rows] = k_pair
            ktbuf[g, :, 0:rows] = k_pair.T
            e_sum = orb_energy(x) + orb_energy(y)
            tot = jnp.zeros((16, WIDE), jnp.float32)
            for r0 in range(0, rows, 16):
                rs = pl.ds(r0, 16)
                k, kt = kbuf[g, rs, :], ktbuf[g, rs, :]
                rec = 1.0 / (e_sum - vmat[rs, :])
                if weight is not None and g in weight:
                    rec = rec * weight[g]
                t, tt = k * rec, kt * rec
                w, wt = (t + t) - tt, (tt + tt) - t
                tot = tot + k * w
                ucat[rs, c0:c0 + WIDE] = t.astype(jnp.bfloat16)
                wcat[pl.ds(c0 + r0, 16), :] = wt.astype(jnp.bfloat16)
                if g not in diag:
                    c1 = c0 + WIDE
                    ucat[rs, c1:c1 + WIDE] = tt.astype(jnp.bfloat16)
                    wcat[pl.ds(c1 + r0, 16), :] = w.astype(jnp.bfloat16)
            c0 += WIDE if g in diag else 2 * WIDE
            fold = tot[0:8, 0:LANES] + tot[8:16, 0:LANES] + tot[0:8, LANES:WIDE] + tot[8:16, LANES:WIDE]
            eacc[x] = eacc[x] + fold
            if g not in diag:
                eacc[y] = eacc[y] + fold
        dacc[...] = dacc[...] + jnp.dot(ucat[:, 0:c0], wcat[0:c0, :], preferred_element_type=jnp.float32)

    extra = nv - LANES
    tiles = nb + 1
    band = tiles * LANES
    side = nb * LANES
    lane128 = lax.broadcasted_iota(jnp.int32, (1, LANES), 1)

    def in_band(j):
        return (lane128 >= j * extra) & (lane128 < (j + 1) * extra)

    def pack_rows(which, s0):
        for n in range(nb):
            ypt[which, :, n * LANES:(n + 1) * LANES] = blk[s0 + n, 0:LANES, :].astype(jnp.float32).T.astype(jnp.bfloat16)
        rests = [blk[s0 + n, LANES:rows, :].astype(jnp.float32)[0:extra] for n in range(nb)]
        rests.append(jnp.zeros((LANES - nb * extra, deep), jnp.float32))
        ypt[which, :, side:band] = jnp.concatenate(rests, axis=0).T.astype(jnp.bfloat16)

    def late_group(g, x, s0):
        kp[g] = jnp.dot(blk[x], ypt[g], preferred_element_type=jnp.float32)
        side_t = kp[g, 0:LANES, side:band].T
        for n in range(nb):
            at = pl.ds(n * LANES, LANES)
            ktp[g, 0:LANES, at] = kp[g, 0:LANES, at].T
            ktp[g, LANES:nv, at] = side_t[n * extra:(n + 1) * extra]
        low = [kp[g, LANES:nv, n * LANES:(n + 1) * LANES] for n in range(nb)]
        low.append(jnp.zeros((LANES - nb * extra, LANES), jnp.float32))
        ktp[g, 0:LANES, side:band] = jnp.concatenate(low, axis=0).T
        corner = kp[g, LANES:nv, side:band]
        corner_t = jnp.concatenate([corner, jnp.zeros((LANES - extra, LANES), jnp.float32)], axis=0).T
        spread = corner_t[0:extra]
        for n in range(1, nb):
            spread = spread + pltpu.roll(corner_t[n * extra:(n + 1) * extra], n * extra, 1)
        ktp[g, LANES:nv, side:band] = spread
        e_x = orb_energy(x)
        e_sums = [e_x + orb_energy(s0 + n) for n in range(nb)]
        e_rest = jnp.full((1, LANES), e_sums[nb - 1], jnp.float32)
        for n in range(nb - 1):
            e_rest = jnp.where(in_band(n), e_sums[n], e_rest)
        tots = [jnp.zeros((16, LANES), jnp.float32) for _ in range(tiles)]
        c0 = 2 * g * band
        for r0 in range(0, rows, 16):
            rs = pl.ds(r0, 16)
            for n in range(tiles):
                k, kt = kp[g, rs, n * LANES:(n + 1) * LANES], ktp[g, rs, n * LANES:(n + 1) * LANES]
                den = e_rest - vrest[rs, :] if n == nb else e_sums[n] - vmat[rs, 0:LANES]
                rec = 1.0 / den
                t, tt = k * rec, kt * rec
                w, wt = (t + t) - tt, (tt + tt) - t
                tots[n] = tots[n] + k * w
                c = c0 + n * LANES
                up[rs, c:c + LANES] = t.astype(jnp.bfloat16)
                wp[rs, c:c + LANES] = w.astype(jnp.bfloat16)
                up[rs, c + band:c + band + LANES] = tt.astype(jnp.bfloat16)
                wp[rs, c + band:c + band + LANES] = wt.astype(jnp.bfloat16)
        folds = [q[0:8] + q[8:16] for q in tots]
        eacc[x] = eacc[x] + sum(folds)
        for n in range(nb):
            eacc[s0 + n] = eacc[s0 + n] + folds[n] + jnp.where(in_band(n), folds[nb], 0.0)

    vside = vmat[:, LANES:WIDE]
    vmix = jnp.ones((rows, LANES), jnp.float32)
    for n in range(nb):
        vmix = jnp.where(in_band(n), vside if n == 0 else pltpu.roll(vside, n * extra, 1), vmix)
    vrest[...] = vmix
    ktp[...] = jnp.zeros_like(ktp)

    ring = nb // 2
    work([(own0 + i, own0 + i) for i in range(nb)]
         + [(own0 + i, own0 + (i + d) % nb) for d in range(1, ring + 1) for i in range(nb)], diag=range(nb))

    to_s[0].wait_recv()
    unpack(3, sib0)
    to_s[1].wait_recv()

    def sib_pair(i, d):
        j = lax.rem(i + d, nb)
        return own0 + jnp.where(core == 0, i, j), sib0 + jnp.where(core == 0, j, i)

    shift = jnp.where(core == 0, 0, ring + 1)
    cut = (nb + 1) // 2
    rest = [(jnp.where(core == 0, i, jnp.minimum(cut + i, nb - 1)), ring) for i in range(cut)]
    work([sib_pair(i, d + shift) for d in range(ring) for i in range(nb)] + [sib_pair(i, d) for i, d in rest],
         weight={ring * nb + cut - 1: jnp.where(core == 0, 1.0, 0.0)})

    def arrive(late, s):
        remote(cols(own0), cols(e0 + late * nb + s), nbr_send.at[0, s], nbr_sem.at[late, s], n_dst).wait_recv()

    def arrive_rest(late):
        remote(pack.at[0], pack.at[1 + late], nbr_send.at[0, nb], nbr_sem.at[late, nb], n_dst).wait_recv()
        unpack(1 + late, e0 + late * nb)

    def with_own(slot):
        return [(own0 + i, slot) for i in range(nb)]

    head = nb // 2
    pack_rows(0, own0)
    arrive_rest(0)
    for s in range(head):
        arrive(0, s)
    work([q for s in range(head) for q in with_own(e0 + s)])
    arrive(0, head)
    work(with_own(e0 + head))
    launch(to_n[0:nb], jnp.logical_not(n_early))
    launch(to_p[0:nb], jnp.logical_not(p_early))

    for s in range(head + 1, nb):
        arrive(0, s)
    work([q for s in range(head + 1, nb) for q in with_own(e0 + s)])
    arrive_rest(1)

    pack_rows(1, e0)

    def late_step(j, _):
        arrive(1, j)
        late_group(0, l0 + j, own0)
        late_group(1, l0 + j, e0)
        dacc[:, 0:rows] = dacc[:, 0:rows] + lax.dot_general(up[...], wp[...], (((1,), (1,)), ((), ())),
                                                            preferred_element_type=jnp.float32)
        return 0

    lax.fori_loop(0, nb, late_step, 0)

    stack = 32
    part[0:nv, :] = dacc[0:nv, 0:LANES]
    rest = dacc[:, LANES:WIDE]
    mix = rest[0:stack]
    for g in range(1, rows // stack):
        mix = mix + pltpu.roll(rest[g * stack:(g + 1) * stack], g * extra, 1)
    part[nv:nv + stack, :] = mix

    half = red_ref.shape[0] // CORES
    mine, other = pl.ds(core * half, half), pl.ds(flip(core, 1) * half, half)
    swap = remote(part.at[other], rbuf, red_send.at[0], red_recv.at[0], sib)
    swap.start()
    es, sums = [], []
    hops = sorted(range(1, n_chip), key=lambda r: -min(r, n_chip - r))
    swap.wait_recv()
    hbuf[chip] = part[mine, :] + rbuf[...]
    for r in hops:
        dst = lax.rem(chip + r, n_chip) * CORES + core
        sums.append(remote(hbuf.at[chip], hbuf.at[chip], red_send.at[r], red_recv.at[r], dst))
        sums[-1].start()

    lane1 = lax.broadcasted_iota(jnp.int32, (1, LANES), 1)
    erow = jnp.zeros((1, LANES), jnp.float32)
    for kind, dev in enumerate((me, sib, e_src, l_src)):
        for s in range(nb):
            e_val = jnp.sum(jnp.sum(eacc[kind * nb + s], axis=0, keepdims=True), axis=1, keepdims=True)
            erow = erow + jnp.where(lane1 == dev * nb + s, e_val, 0.0)
    elocal[...] = erow
    for r in range(1, n_dev):
        es.append(remote(elocal, ebuf.at[r - 1], e_send.at[r - 1], e_recv.at[r - 1], lax.rem(me + r, n_dev)))
        es[-1].start()

    for c in to_n + to_p + to_s + [swap]:
        c.wait_send()
    for r in range(1, n_chip):
        src = lax.rem(chip + n_chip - r, n_chip)
        remote(hbuf.at[chip], hbuf.at[src], red_send.at[r], red_recv.at[r], src * CORES + core).wait_recv()
    total = hbuf[0]
    for r in range(1, n_chip):
        total = total + hbuf[r]
    red_ref[mine, :] = total
    back = remote(red_ref.at[mine], red_ref.at[mine], gat_send, gat_recv, sib)
    back.start()
    for c in es:
        c.wait_recv()
    place = lax.rem(me, n_dev)
    e_all = jnp.zeros((1, LANES), jnp.float32)
    for d in range(n_dev):
        took = elocal[...]
        for r in range(1, n_dev):
            took = jnp.where(lax.rem(place + n_dev - r, n_dev) == d, ebuf[r - 1], took)
        e_all = e_all + took
    e_ref[0:1, :] = pltpu.roll(jnp.broadcast_to(e_all, (8, LANES)), lax.rem(LANES - me * nb, LANES), 1)[0:1]
    e_ref[1:2, :] = jnp.broadcast_to(jnp.sum(e_all, axis=1, keepdims=True), (1, LANES))
    for c in sums + es + [back]:
        c.wait_send()
    remote(red_ref.at[mine], red_ref.at[other], gat_send, gat_recv, sib).wait_recv()


def finish(nb, nv, red_ref, e_ref, dens_ref, epair_ref, energy_ref):
    extra, stack = nv - LANES, 32
    dens_ref[:, 0:LANES] = red_ref[0:nv, :]
    mix = red_ref[nv:nv + stack, :]
    for g in range(-(-nv // stack)):
        n = min(stack, nv - g * stack)
        side = mix if g == 0 else pltpu.roll(mix, LANES - g * extra, 1)
        dens_ref[g * stack:g * stack + n, LANES:nv] = side[0:n, 0:extra]
    epair_ref[...] = e_ref[0:1, 0:nb]
    energy_ref[...] = e_ref[1:2, 0:1]


def solution(mesh):
    n_dev = mesh.shape['occ']

    def per_device(b_blk, eps_occ, eps_vir):
        nq, nb, nv = b_blk.shape
        rows = (nv + 15) // 16 * 16
        n_cut = -(-(nv + 32) // n_dev)
        cut_rows = (n_cut + 7) // 8 * 8
        deep = (nq + LANES - 1) // LANES * LANES
        most = 3 * nb
        by_orb = jnp.transpose(b_blk, (1, 2, 0))
        vmem = pltpu.VMEM
        dma = pltpu.SemaphoreType.DMA
        f32, bf16 = jnp.float32, jnp.bfloat16
        anyspace = pl.BlockSpec(memory_space=pl.ANY)
        in_vmem = pl.BlockSpec(memory_space=vmem)
        red, e_rows = pl.pallas_call(
            functools.partial(kernel, n_dev, nb, nv, nq),
            out_shape=(jax.ShapeDtypeStruct((n_dev * cut_rows, LANES), f32), jax.ShapeDtypeStruct((8, LANES), f32)),
            in_specs=[anyspace] * 3,
            out_specs=(in_vmem,) * 2,
            scratch_shapes=[
                vmem((4 * nb, rows, deep), bf16),
                vmem((nb, nv, nq % LANES), bf16),
                vmem((4, nb, rows // (LANES // (nq % LANES)), LANES), bf16),
                pltpu.SMEM((nb * n_dev,), f32),
                vmem((1, nv), f32),
                vmem((most, rows, WIDE), f32),
                vmem((most, rows, WIDE), f32),
                vmem((rows, 2 * most * WIDE), bf16),
                vmem((2 * most * WIDE, WIDE), bf16),
                vmem((rows, WIDE), f32),
                vmem((4 * nb, 8, LANES), f32),
                vmem((rows, WIDE), f32),
                vmem((n_dev * cut_rows, LANES), f32),
                vmem((n_dev * cut_rows // CORES, LANES), f32),
                vmem((n_dev // CORES, n_dev * cut_rows // CORES, LANES), f32),
                vmem((n_dev - 1, 1, LANES), f32),
                vmem((1, LANES), f32),
                vmem((2, deep, (nb + 1) * LANES), bf16),
                vmem((2, rows, (nb + 1) * LANES), f32),
                vmem((2, rows, (nb + 1) * LANES), f32),
                vmem((rows, 4 * (nb + 1) * LANES), bf16),
                vmem((rows, 4 * (nb + 1) * LANES), bf16),
                vmem((rows, LANES), f32),
                dma((4,)), dma((2, 2)), dma((2, nb + 1)), dma((2, nb + 1)),
                dma((n_dev // CORES,)), dma((n_dev // CORES,)), dma, dma, dma((n_dev - 1,)), dma((n_dev - 1,)),
            ],
            compiler_params=pltpu.CompilerParams(collective_id=0, has_side_effects=True),
        )(by_orb, eps_occ, eps_vir.reshape(1, nv))
        dens, e_pair, energy = pl.pallas_call(
            functools.partial(finish, nb, nv),
            out_shape=(jax.ShapeDtypeStruct((nv, nv), f32), jax.ShapeDtypeStruct((1, nb), f32), jax.ShapeDtypeStruct((1, 1), f32)),
            in_specs=[in_vmem] * 2,
            out_specs=(in_vmem,) * 3,
        )(red, e_rows)
        return e_pair.reshape(nb), energy.reshape(1), dens

    return jax.shard_map(per_device, mesh=mesh, in_specs=(P(None, ('mol', 'occ'), None), P('mol'), P('mol')),
                         out_specs=(P(('mol', 'occ')), P('mol'), P('mol', None)), check_vma=False)
```
